32 devices in a mesh: dp: 8 (over y, x, core), mp: 4 (over z).
Axes of the slice: x: 2, y: 2, z: 4, core: 2. Of those that a mesh axis runs over, the one named last changes fastest.
Arguments:
- feature_ids: int32 [8, 2048, 8], P('dp'), may hold values from 0 to 4095
- tables: bfloat16 [8, 4096, 128], P('dp'), may hold values from -5 to 5
- table_of_feature: int32 [8], replicated, may hold values from 0 to 7, each once
- cross_down: bfloat16 [2, 1024, 512], P(None, 'mp'), may hold values from -0.1875 to 0.1875
- cross_up: bfloat16 [2, 1024, 512], P(None, 'mp'), may hold values from -0.125 to 0.125
- cross_bias: float32 [2, 1024], P(None, 'mp'), may hold values from -3 to 3
- tower_weight: bfloat16 [1024, 2048], P('dp', 'mp'), may hold values from -0.1875 to 0.1875
- tower_bias: float32 [2048], P('mp'), may hold values from -3 to 3
Outputs:
- hidden: bfloat16 [2048, 2048], P('dp', 'mp')
The draws below stay inside these ranges and needn't reach their ends.
Inputs may be any that keep to these rules, and one draw needn't show every extreme that they name: `feature_ids`: each id indexes a row of its own table. `table_of_feature`: each table serves exactly one feature.
All inputs are finite; a program needn't handle non-finite values.
Results may differ from the reference program's by a relative error of at most 0.015.
Values may be sent and summed in bfloat16 or wider, within the bound.
A program may use at most 64 MiB of HBM per device.

```python
import math
import jax
import jax.numpy as jnp
import numpy as np
from jax import lax

EMBED = 128
RANK = 512
HID = 2048
VOCAB = 4096
HOTS = 8
LAYERS = 2
FEATS = 8
WIDTH = 1024
BATCH = 2048


def touch_ends(result, key, smallest, top_value):
    dims = result.shape
    index_at = [jax.random.randint(jax.random.fold_in(key, axis), (), 0, dims[axis]) for axis in range(len(dims))]
    result = result.at[tuple(index_at)].set(smallest)
    longest = dims.index(max(dims))
    index_at[longest] = (index_at[longest] + 1) % dims[longest]
    return result.at[tuple(index_at)].set(top_value)


def block_scale(stream_key, dims, split, least, largest):
    gain = 1.0
    for position, parts in split:
        draws = jax.random.uniform(jax.random.fold_in(jax.random.fold_in(stream_key, 6), position), (parts,), jnp.float32, least / len(split), largest / len(split))
        gain = gain * jnp.repeat(jnp.exp(draws), dims[position] // parts).reshape((-1,) + (1,) * (len(dims) - 1 - position))
    return gain


def cumulative_ranks(number_of, skew):
    portions = [(1 << 20) // math.isqrt(standing ** skew) + 1 for standing in range(1, number_of + 1)]
    width = 1 + sum(portions) // (1 << 30)
    return np.cumsum(np.array([max(1, weight // width) for weight in portions]))


def ranked(key, extent, count, skew):
    table = cumulative_ranks(count, skew)
    pick = jax.random.randint(jax.random.fold_in(key, 1), extent, 0, int(table[count - 1]))
    rank = jnp.searchsorted(jnp.asarray(table, jnp.int32), pick, side="right")
    return jax.random.permutation(jax.random.fold_in(key, 2), count)[rank].astype(jnp.int32)


def centred(key, extent, deviation, limit, shards=(), held_as=jnp.bfloat16):
    loudness = block_scale(key, extent, shards, -0.22, 0.18) if shards else 1.0
    result = jax.random.normal(key, extent, jnp.float32) * deviation * loudness
    return jnp.minimum(jnp.maximum(result, -limit), limit).astype(held_as)


def setup_inputs(seed: int = 0) -> dict:
    key_list = jax.random.split(jax.random.key(seed), 9)
    return {
        "feature_ids": touch_ends(ranked(key_list[0], (FEATS, BATCH, HOTS), VOCAB, 2), jax.random.fold_in(key_list[0], 3), 0, VOCAB - 1).astype(jnp.int32),
        "tables": centred(key_list[1], (FEATS, VOCAB, EMBED), 0.35, 5.0, ((0, 8),)),
        "table_of_feature": jax.random.permutation(key_list[2], FEATS).astype(jnp.int32),
        "cross_down": centred(key_list[3], (LAYERS, WIDTH, RANK), WIDTH ** -0.5, 0.1875, ((1, 4),)),
        "cross_up": centred(key_list[4], (LAYERS, WIDTH, RANK), (4 * RANK) ** -0.5, 0.125, ((1, 4),)),
        "cross_bias": centred(key_list[5], (LAYERS, WIDTH), 0.5, 3.0, ((1, 4),), jnp.float32),
        "tower_weight": centred(key_list[6], (WIDTH, HID), WIDTH ** -0.5, 0.1875, ((0, 8), (1, 4))),
        "tower_bias": centred(key_list[7], (HID,), 0.5, 3.0, ((0, 4),), jnp.float32),
    }


def pool_table(pair):
    table, id_rows = pair
    summed = jnp.zeros((id_rows.shape[0], table.shape[1]), jnp.float32)
    for hot_index in range(HOTS):
        summed = summed + jnp.take(table, id_rows[:, hot_index], axis=0).astype(jnp.float32)
    return summed.astype(jnp.bfloat16)


def reference(feature_ids, tables, table_of_feature, cross_down, cross_up, cross_bias, tower_weight, tower_bias):
    pooled = lax.map(pool_table, (tables, feature_ids))
    ordered = jnp.take(pooled, table_of_feature, axis=0)
    embedded = jnp.transpose(ordered, (1, 0, 2)).reshape(BATCH, WIDTH)
    embedded_wide = embedded.astype(jnp.float32)
    crossed = embedded
    for layer_index in range(LAYERS):
        projected = jnp.dot(crossed, cross_down[layer_index], preferred_element_type=jnp.float32).astype(jnp.bfloat16)
        lifted = lax.dot_general(projected, cross_up[layer_index], (((1,), (1,)), ((), ())), preferred_element_type=jnp.float32)
        crossed = (embedded_wide * (lifted + cross_bias[layer_index]) + crossed.astype(jnp.float32)).astype(jnp.bfloat16)
    pre_act = jnp.dot(crossed, tower_weight, preferred_element_type=jnp.float32) + tower_bias
    return jax.nn.relu(pre_act).astype(jnp.bfloat16)
```

```python
import functools

import jax
import jax.numpy as jnp
from jax import lax
from jax.experimental import pallas as pl
from jax.experimental.pallas import tpu as pltpu
from jax.sharding import PartitionSpec as P


def plain_body(
    feature_ids,
    tables,
    table_of_feature,
    cross_down,
    cross_up,
    cross_bias,
    tower_weight,
    tower_bias,
):
    groups = lax.axis_size("dp")
    members = lax.axis_size("mp")
    member = lax.axis_index("mp")
    table_count, batch_size, hot_count = feature_ids.shape
    row_count = batch_size // (groups * members)
    shaped = feature_ids[0].reshape(groups, members, row_count, hot_count)
    own_ids = lax.dynamic_index_in_dim(shaped, member, 1, keepdims=False).reshape(
        groups * row_count, hot_count
    )
    summed = jnp.zeros((groups * row_count, tables.shape[2]), jnp.float32)
    for hot_index in range(hot_count):
        summed = summed + jnp.take(tables[0], own_ids[:, hot_index], axis=0).astype(jnp.float32)
    columns = [summed.astype(jnp.bfloat16)]
    pooled = jnp.stack(columns, axis=1)
    regrouped = lax.all_to_all(pooled, "dp", split_axis=0, concat_axis=1, tiled=True)
    ordered = jnp.take(regrouped, table_of_feature, axis=1)
    by_width = lax.all_to_all(ordered, "mp", split_axis=1, concat_axis=0, tiled=True)
    group_rows = by_width.shape[0]
    embedded = by_width.reshape(group_rows, -1)
    embedded_wide = embedded.astype(jnp.float32)
    crossed = embedded
    layer_total = cross_down.shape[0]
    for layer_index in range(layer_total):
        partial_value = jnp.dot(
            crossed, cross_down[layer_index], preferred_element_type=jnp.float32
        )
        projected = lax.psum(partial_value.astype(jnp.bfloat16), "mp")
        lifted = lax.dot_general(
            projected,
            cross_up[layer_index],
            (((1,), (1,)), ((), ())),
            preferred_element_type=jnp.float32,
        )
        crossed = (
            embedded_wide * (lifted + cross_bias[layer_index]) + crossed.astype(jnp.float32)
        ).astype(jnp.bfloat16)
    full_rows = lax.all_gather(crossed, "mp", axis=1, tiled=True)
    pre_act = jnp.dot(
        full_rows,
        lax.all_gather(tower_weight, "dp", axis=0, tiled=True),
        preferred_element_type=jnp.float32,
    )
    return jax.nn.relu(pre_act + tower_bias).astype(jnp.bfloat16)


MESH = pl.DeviceIdType.MESH
KERNEL_BYTES = 24 * 1024 * 1024
VMEM_BYTES = (64 * 1024 - 352) * 1024
CHIPS = 4
PLANES = 4
STEPS = (1, 3, 2)


def kernel(
    groups,
    members,
    ids_hbm,
    order_hbm,
    table,
    down,
    up,
    bias,
    tower,
    tower_bias_hbm,
    out,
    ids,
    order,
    table_half,
    table_wide,
    sums,
    outbox,
    pooled,
    embedded,
    crossed,
    weights,
    biases,
    tower_all,
    tower_bias,
    local_sem,
    send_sem,
    z_recv,
    plane_recv,
    diag_recv,
    pair_recv,
    tower_recv,
    pool_recv,
    share_recv,
    bias_recv,
):
    d = lax.axis_index("dp")
    m = lax.axis_index("mp")
    q = lax.div(d, 2)
    c = lax.rem(d, 2)
    partner = q * 2 + 1 - c
    chip_x = q + 1 - 2 * lax.rem(q, 2)
    chip_y = lax.rem(q + 2, CHIPS)
    chip_z = lax.rem(chip_x + 2, CHIPS)
    chips = (chip_x, chip_y, chip_z)
    layers, block, rank = down.shape
    hots = ids.shape[0]
    rows, embed = sums.shape
    piece = block // groups
    depth = tower.shape[0]
    pieces = 2 * layers
    others = members - 1

    def wrap(value, size):
        return lax.rem(value + size, size)

    def load(src, dst, index):
        copy = pltpu.make_async_copy(src, dst, local_sem.at[index])
        copy.start()
        return copy

    def remote(src, dst, which, recv_sem, to_d, to_m):
        return pltpu.make_async_remote_copy(
            src_ref=src,
            dst_ref=dst,
            send_sem=send_sem.at[which],
            recv_sem=recv_sem,
            device_id=(to_d, to_m),
            device_id_type=MESH,
        )

    def send(src, dst, which, recv_sem, to_d, to_m):
        remote(src, dst, which, recv_sem, to_d, to_m).start()

    def arrived(ref, recv_sem):
        remote(ref, ref, 0, recv_sem, partner, m).wait_recv()

    def came(k):
        return wrap(m - k, members)

    def goes(k):
        return wrap(m + k, members)

    def slot(p, member, device, half=None):
        length = piece if half is None else piece // 2
        start = member * block + device * piece + (0 if half is None else half * length)
        return weights.at[p, pl.ds(pl.multiple_of(start, length), length), :]

    def tower_slot(device, half=None):
        length = depth if half is None else depth // 2
        start = device * depth + (0 if half is None else half * length)
        return tower_all.at[pl.ds(pl.multiple_of(start, length), length), :]

    def source(p):
        return (down, up)[p % 2].at[p // 2]

    barrier = pltpu.get_barrier_semaphore()
    for k in range(1, members):
        pl.semaphore_signal(barrier, inc=1, device_id=(d, goes(k)), device_id_type=MESH)
    for i in range(1, groups):
        pl.semaphore_signal(barrier, inc=1, device_id=(wrap(d + i, groups), m), device_id_type=MESH)

    here = pl.ds(pl.multiple_of(m * block, block), block)
    own = pl.ds(pl.multiple_of(d * piece, piece), piece)
    tower_copy = load(tower, tower_slot(d), 0)
    weight_copies = [load(source(p), weights.at[p, here, :], 1 + p) for p in range(pieces)]
    table_copy = load(table.at[0], table_half, pieces + 1)
    ids_copy = load(ids_hbm, ids, pieces + 2)
    bias_copy = load(bias, biases.at[m], pieces + 3)
    order_copy = load(order_hbm, order, pieces + 4)
    tower_bias_copy = load(tower_bias_hbm, tower_bias, pieces + 5)

    def lend(p):
        for k in STEPS:
            mine = slot(p, m, d)
            send(mine, mine, 0, z_recv.at[p, k - 1], d, goes(k))

    def spread(p, k):
        mine = slot(p, came(k), d)
        arrived(mine, z_recv.at[p, k - 1])
        send(mine, mine, 0, plane_recv.at[p, k - 1], chip_x * 2 + c, m)
        send(mine, mine, 0, plane_recv.at[p, k - 1], chip_y * 2 + c, m)
        send(mine, mine, 0, pair_recv.at[p, k - 1], partner, m)

    def relay(p, k):
        arrived(weights.at[p, pl.ds(0, 2 * piece), :], plane_recv.at[p, k - 1])
        for j in range(2):
            half = slot(p, came(k), chips[j] * 2 + c, j)
            send(half, half, 0, diag_recv.at[p, k - 1], chips[1 - j] * 2 + c, m)
        for j in range(2):
            whole = slot(p, came(k), chips[j] * 2 + c)
            send(whole, whole, 0, pair_recv.at[p, k - 1], partner, m)

    def corner(p, k):
        far = slot(p, came(k), chip_z * 2 + c)
        arrived(far, diag_recv.at[p, k - 1])
        send(far, far, 0, pair_recv.at[p, k - 1], partner, m)

    def complete(p, k):
        arrived(weights.at[p, pl.ds(0, CHIPS * piece), :], pair_recv.at[p, k - 1])

    def tower_spread():
        mine = tower_slot(d)
        send(mine, mine, 1, tower_recv.at[0], chip_x * 2 + c, m)
        send(mine, mine, 1, tower_recv.at[0], chip_y * 2 + c, m)
        send(mine, mine, 1, tower_recv.at[2], partner, m)

    def tower_relay():
        arrived(tower_all.at[pl.ds(0, 2 * depth), :], tower_recv.at[0])
        for j in range(2):
            half = tower_slot(chips[j] * 2 + c, j)
            send(half, half, 1, tower_recv.at[1], chips[1 - j] * 2 + c, m)
        for j in range(2):
            whole = tower_slot(chips[j] * 2 + c)
            send(whole, whole, 1, tower_recv.at[2], partner, m)

    def tower_corner():
        far = tower_slot(chip_z * 2 + c)
        arrived(far, tower_recv.at[1])
        send(far, far, 1, tower_recv.at[2], partner, m)

    step = 16 if rows % 16 == 0 else 8

    def pool(group):
        first = pl.multiple_of((group * members + m) * rows, rows)

        def some(index, carry):
            base = pl.multiple_of(index * step, step)
            for r in range(step):
                total = None
                for hot in range(hots):
                    at = ids[hot, first + base + r]
                    row = table_wide[pl.ds(at, 1), :]
                    total = row if total is None else total + row
                sums[pl.ds(base + r, 1), :] = total
            return carry

        lax.fori_loop(0, rows // step, some, 0)
        return sums[...].astype(jnp.bfloat16)

    def pool_out(i):
        if i == 0:
            pooled[m, d] = pool(d)
        else:
            outbox[i] = pool(wrap(d + i, groups))

    def pool_away(i):
        send(outbox.at[i], pooled.at[m, d], 2, pool_recv.at[0], wrap(d + i, groups), m)

    half_of = lax.div(m, 2)
    beside = m + 1 - 2 * lax.rem(m, 2)
    across = 2 - half_of
    far_first = 2 * (1 - half_of)
    inner = jnp.logical_or(m == 1, m == 2)

    def share():
        arrived(outbox.at[pl.ds(0, groups - 1)], pool_recv.at[0])
        mine = pooled.at[m]
        send(mine, mine, 3, share_recv.at[m], d, across)
        send(mine, mine, 3, share_recv.at[m], d, beside)

    def pass_on():
        @pl.when(inner)
        def _():
            for quarter in (3 - m, m + 2 - 4 * half_of):
                theirs = pooled.at[quarter]
                arrived(theirs, share_recv.at[quarter])
                send(theirs, theirs, 3, share_recv.at[quarter], d, beside)

    def shared():
        arrived(pooled.at[beside], share_recv.at[beside])

        @pl.when(jnp.logical_not(inner))
        def _():
            for j in range(2):
                arrived(pooled.at[far_first + j], share_recv.at[far_first + j])

    def matching(p, b):
        return weights[p, pl.ds(pl.multiple_of(b * block, block), block), :]

    def embed_all():
        per_block = block // embed
        order_copy.wait()
        for b in range(members):
            for f in range(per_block):
                at = order[b * per_block + f]
                for quarter in range(members):
                    embedded[
                        b, quarter * rows : (quarter + 1) * rows, f * embed : (f + 1) * embed
                    ] = pooled[quarter, at]

    def project(layer):
        state = embedded if layer == 0 else crossed
        for k in STEPS:
            complete(2 * layer, k)
        value = None
        for b in range(members):
            term = jnp.dot(
                state[b],
                weights[2 * layer, b * block : (b + 1) * block, :],
                preferred_element_type=jnp.float32,
            )
            value = term if value is None else value + term
        return value.astype(jnp.bfloat16)

    def lift(layer, projected, b):
        state = embedded if layer == 0 else crossed
        lifted = lax.dot_general(
            projected,
            matching(2 * layer + 1, b),
            (((1,), (1,)), ((), ())),
            preferred_element_type=jnp.float32,
        )
        wide = embedded[b].astype(jnp.float32)
        value = wide * (lifted + biases[b, layer : layer + 1, :]) + state[b].astype(jnp.float32)
        return value.astype(jnp.bfloat16)

    units = [(p, k) for p in range(pieces) for k in STEPS]

    def at_scope(name, call, *args):
        with jax.named_scope(name):
            return call(*args)

    def do(call, *args):
        return at_scope(call.__name__ + "_".join(map(str, args)), call, *args)

    def first_sends():
        tower_copy.wait()
        for copy in weight_copies:
            copy.wait()
        bias_copy.wait()
        pl.semaphore_wait(barrier, members - 1 + groups - 1)

    do(first_sends)
    tower_spread()
    lend(0)
    for k in range(1, members):
        send(biases.at[m], biases.at[m], 4, bias_recv.at[0], d, goes(k))
    lend(1)

    def widen():
        table_copy.wait()
        table_wide[...] = table_half[...].astype(jnp.float32)
        ids_copy.wait()

    do(widen)
    jobs = {
        3: [(spread, *units[0])],
        4: [(spread, *units[1])],
        5: [(spread, *units[2]), (tower_relay,)],
        6: [(relay, *units[0]), (spread, *units[3])],
        7: [(relay, *units[1]), (spread, *units[4])],
        8: [(tower_corner,), (relay, *units[2])],
    }
    for turn in range(1, groups + 1):
        i = turn % groups
        do(pool_out, i)
        if turn > 1:
            pool_away(turn - 1)
        for job in jobs.get(turn, []):
            do(*job)
    do(share)
    lend(2)
    lend(3)
    spread_done, relay_done, corner_done = 5, 3, 0

    def upto(kind, done, count):
        for unit in units[done:count]:
            do(kind, *unit)
        return count

    def advance(target):
        nonlocal spread_done, relay_done, corner_done
        while spread_done < min(target, len(units)):
            spread_done = upto(spread, spread_done, spread_done + 1)
            relay_done = upto(relay, relay_done, max(relay_done, spread_done - 2))
            corner_done = upto(corner, corner_done, max(corner_done, spread_done - 4))

    advance(7)
    do(pass_on)
    advance(9)
    do(shared)
    do(embed_all)
    corner_done = upto(corner, corner_done, max(corner_done, 3))
    arrived(biases.at[pl.ds(0, others)], bias_recv.at[0])
    projected = do(project, 0)
    advance(11)
    corner_done = upto(corner, corner_done, max(corner_done, 6))
    for k in (0,) + STEPS:
        if k:
            do(complete, 1, k)
        b = came(k)
        crossed[b] = lift(0, projected, b)
    advance(12)
    relay_done = upto(relay, relay_done, 11)
    corner_done = upto(corner, corner_done, 9)
    projected = do(project, 1)
    relay_done = upto(relay, relay_done, 12)
    tower_bias_copy.wait()
    arrived(tower_all.at[pl.ds(0, CHIPS * depth), :], tower_recv.at[2])
    answer = None
    for k in (0,) + STEPS:
        if k:
            do(corner, pieces - 1, k)
            do(complete, pieces - 1, k)
        b = came(k)
        value = lift(1, projected, b)
        part = jnp.dot(
            value,
            tower_all[pl.ds(pl.multiple_of(b * block, block), block), :],
            preferred_element_type=jnp.float32,
        )
        answer = part if answer is None else answer + part
    out[...] = jnp.maximum(answer + tower_bias[...], 0.0).astype(jnp.bfloat16)

    def sent(ref, which):
        remote(ref, ref, which, bias_recv.at[0], partner, m).wait_send()

    def all_sent():
        sent(weights.at[:, pl.ds(0, others * block), :], 0)
        sent(tower_all.at[pl.ds(0, 7 * depth), :], 1)
        sent(outbox.at[pl.ds(0, groups - 1)], 2)
        sent(pooled.at[pl.ds(0, 2)], 3)

        @pl.when(inner)
        def _():
            sent(pooled.at[pl.ds(0, 2)], 3)

        sent(biases.at[pl.ds(0, others)], 4)

    do(all_sent)


def fused_body(
    feature_ids,
    tables,
    table_of_feature,
    cross_down,
    cross_up,
    cross_bias,
    tower_weight,
    tower_bias,
):
    groups = lax.axis_size("dp")
    members = lax.axis_size("mp")
    _, batch_size, hot_count = feature_ids.shape
    rows = batch_size // (groups * members)
    _, vocab, embed = tables.shape
    layers, block, rank = cross_down.shape
    depth, units = tower_weight.shape
    width = block * members
    pieces = 2 * layers
    dma = pltpu.SemaphoreType.DMA
    anywhere = pl.BlockSpec(memory_space=pl.ANY)
    vmem = pl.BlockSpec(memory_space=pltpu.VMEM)
    return pl.pallas_call(
        functools.partial(kernel, groups, members),
        out_shape=pltpu.VMEM((rows * members, units), jnp.bfloat16),
        in_specs=[anywhere] * 8,
        out_specs=vmem,
        scratch_shapes=[
            pltpu.SMEM((hot_count, batch_size), jnp.int32),
            pltpu.SMEM(table_of_feature.shape, jnp.int32),
            pltpu.VMEM((vocab, embed), jnp.bfloat16),
            pltpu.VMEM((vocab, embed), jnp.float32),
            pltpu.VMEM((rows, embed), jnp.float32),
            pltpu.VMEM((groups, rows, embed), jnp.bfloat16),
            pltpu.VMEM((members, groups, rows, embed), jnp.bfloat16),
            pltpu.VMEM((members, rows * members, block), jnp.bfloat16),
            pltpu.VMEM((members, rows * members, block), jnp.bfloat16),
            pltpu.VMEM((pieces, width, rank), jnp.bfloat16),
            pltpu.VMEM((members, layers, block), jnp.float32),
            pltpu.VMEM((width, units), jnp.bfloat16),
            pltpu.VMEM((1, units), jnp.float32),
            dma((6 + pieces,)),
            dma((5,)),
            dma((pieces, members - 1)),
            dma((pieces, members - 1)),
            dma((pieces, members - 1)),
            dma((pieces, members - 1)),
            dma((3,)),
            dma((1,)),
            dma((members,)),
            dma((1,)),
        ],
        compiler_params=pltpu.CompilerParams(
            collective_id=0, has_side_effects=True, vmem_limit_bytes=VMEM_BYTES
        ),
    )(
        feature_ids[0].T,
        table_of_feature,
        tables,
        cross_down,
        cross_up,
        cross_bias,
        tower_weight,
        tower_bias.reshape(1, -1),
    )


def body(
    feature_ids,
    tables,
    table_of_feature,
    cross_down,
    cross_up,
    cross_bias,
    tower_weight,
    tower_bias,
):
    groups = lax.axis_size("dp")
    members = lax.axis_size("mp")
    held = 2 * members * (cross_down.size + cross_up.size) + 2 * groups * tower_weight.size
    placed = groups == 2 * CHIPS and members == PLANES
    fits = held <= KERNEL_BYTES and placed and tables.shape[0] == 1
    chosen = fused_body if fits else plain_body
    return chosen(
        feature_ids,
        tables,
        table_of_feature,
        cross_down,
        cross_up,
        cross_bias,
        tower_weight,
        tower_bias,
    )


def solution(mesh):
    return jax.shard_map(
        body,
        mesh=mesh,
        in_specs=(
            P("dp", None, None),
            P("dp", None, None),
            P(),
            P(None, "mp", None),
            P(None, "mp", None),
            P(None, "mp"),
            P("dp", "mp"),
            P("mp"),
        ),
        out_specs=P("dp", "mp"),
        check_vma=False,
    )
```

```python
import functools

import jax
import jax.numpy as jnp
from jax import lax
from jax.experimental import pallas as pl
from jax.experimental.pallas import tpu as pltpu
from jax.sharding import PartitionSpec as P


def plain_body(
    feature_ids,
    tables,
    table_of_feature,
    cross_down,
    cross_up,
    cross_bias,
    tower_weight,
    tower_bias,
):
    groups = lax.axis_size("dp")
    members = lax.axis_size("mp")
    member = lax.axis_index("mp")
    table_count, batch_size, hot_count = feature_ids.shape
    row_count = batch_size // (groups * members)
    shaped = feature_ids[0].reshape(groups, members, row_count, hot_count)
    own_ids = lax.dynamic_index_in_dim(shaped, member, 1, keepdims=False).reshape(
        groups * row_count, hot_count
    )
    summed = jnp.zeros((groups * row_count, tables.shape[2]), jnp.float32)
    for hot_index in range(hot_count):
        summed = summed + jnp.take(tables[0], own_ids[:, hot_index], axis=0).astype(jnp.float32)
    columns = [summed.astype(jnp.bfloat16)]
    pooled = jnp.stack(columns, axis=1)
    regrouped = lax.all_to_all(pooled, "dp", split_axis=0, concat_axis=1, tiled=True)
    ordered = jnp.take(regrouped, table_of_feature, axis=1)
    by_width = lax.all_to_all(ordered, "mp", split_axis=1, concat_axis=0, tiled=True)
    group_rows = by_width.shape[0]
    embedded = by_width.reshape(group_rows, -1)
    embedded_wide = embedded.astype(jnp.float32)
    crossed = embedded
    layer_total = cross_down.shape[0]
    for layer_index in range(layer_total):
        partial_value = jnp.dot(
            crossed, cross_down[layer_index], preferred_element_type=jnp.float32
        )
        projected = lax.psum(partial_value.astype(jnp.bfloat16), "mp")
        lifted = lax.dot_general(
            projected,
            cross_up[layer_index],
            (((1,), (1,)), ((), ())),
            preferred_element_type=jnp.float32,
        )
        crossed = (
            embedded_wide * (lifted + cross_bias[layer_index]) + crossed.astype(jnp.float32)
        ).astype(jnp.bfloat16)
    full_rows = lax.all_gather(crossed, "mp", axis=1, tiled=True)
    pre_act = jnp.dot(
        full_rows,
        lax.all_gather(tower_weight, "dp", axis=0, tiled=True),
        preferred_element_type=jnp.float32,
    )
    return jax.nn.relu(pre_act + tower_bias).astype(jnp.bfloat16)


MESH = pl.DeviceIdType.MESH
KERNEL_BYTES = 24 * 1024 * 1024
VMEM_BYTES = (64 * 1024 - 352) * 1024
CHIPS = 4
PLANES = 4
STEPS = (1, 3, 2)
PLAN = (
    "flip", "widen", "P1", "P2", "A1", "L1", "P3", "A2", "L3", "P4", "A3", "S0", "S1", "P5",
    "A4", "P6", "A5", "S2", "P7", "A6", "TR", "P0", "A7", "R0", "R1", "S3", "S4", "R2", "S5",
    "SH", "R3", "R4", "S6", "R5", "S7", "S8", "C0", "C1", "C2", "TC", "R6", "S9", "R7", "S10",
    "R8", "S11", "C3", "C4", "C5", "R9", "F1", "R10", "F0", "R11", "C6", "C7", "C8", "E", "X0",
    "Y", "C9", "C10", "C11", "X1", "Z01", "Z32", "end",
)


def kernel(
    groups,
    members,
    ids_hbm,
    order_hbm,
    table,
    down,
    up,
    bias,
    tower,
    tower_bias_hbm,
    out,
    ids,
    order,
    table_half,
    table_wide,
    sums,
    outbox,
    pooled,
    embedded,
    crossed,
    weights,
    up_raw,
    lifts,
    biases,
    tower_all,
    tower_bias,
    local_sem,
    send_sem,
    z_recv,
    plane_recv,
    diag_recv,
    pair_recv,
    tower_recv,
    pool_recv,
    share_recv,
    bias_recv,
):
    d = lax.axis_index("dp")
    m = lax.axis_index("mp")
    q = lax.div(d, 2)
    c = lax.rem(d, 2)
    partner = q * 2 + 1 - c
    chip_x = q + 1 - 2 * lax.rem(q, 2)
    chip_y = lax.rem(q + 2, CHIPS)
    chip_z = lax.rem(chip_x + 2, CHIPS)
    chips = (chip_x, chip_y, chip_z)
    layers, block, rank = down.shape
    hots = ids.shape[0]
    rows, embed = sums.shape
    piece = block // groups
    depth = tower.shape[0]
    pieces = 2 * layers
    others = members - 1

    def wrap(value, size):
        return lax.rem(value + size, size)

    def load(src, dst, index):
        copy = pltpu.make_async_copy(src, dst, local_sem.at[index])
        copy.start()
        return copy

    def remote(src, dst, which, recv_sem, to_d, to_m):
        return pltpu.make_async_remote_copy(
            src_ref=src,
            dst_ref=dst,
            send_sem=send_sem.at[which],
            recv_sem=recv_sem,
            device_id=(to_d, to_m),
            device_id_type=MESH,
        )

    def send(src, dst, which, recv_sem, to_d, to_m):
        remote(src, dst, which, recv_sem, to_d, to_m).start()

    def arrived(ref, recv_sem):
        remote(ref, ref, 0, recv_sem, partner, m).wait_recv()

    def came(k):
        return wrap(m - k, members)

    def goes(k):
        return wrap(m + k, members)

    thin = rank // groups

    def slot(p, member, device, half=None):
        full = piece if p % 2 == 0 else thin
        length = full if half is None else full // 2
        start = device * full + (0 if half is None else half * length)
        if p % 2 == 0:
            start = member * block + start
            return weights.at[p // 2, pl.ds(pl.multiple_of(start, length), length), :]
        return lifts.at[p // 2, member, pl.ds(pl.multiple_of(start, length), length), :]

    def amount(p, count):
        if p % 2 == 0:
            return weights.at[p // 2, pl.ds(0, count * piece), :]
        return lifts.at[p // 2, 0, pl.ds(0, count * thin), :]

    def tower_slot(device, half=None):
        length = depth if half is None else depth // 2
        start = device * depth + (0 if half is None else half * length)
        return tower_all.at[pl.ds(pl.multiple_of(start, length), length), :]

    barrier = pltpu.get_barrier_semaphore()
    for k in range(1, members):
        pl.semaphore_signal(barrier, inc=1, device_id=(d, goes(k)), device_id_type=MESH)
    for i in range(1, groups):
        pl.semaphore_signal(barrier, inc=1, device_id=(wrap(d + i, groups), m), device_id_type=MESH)

    here = pl.ds(pl.multiple_of(m * block, block), block)
    tower_copy = load(tower, tower_slot(d), 0)
    weight_copies = [load(down.at[n], weights.at[n, here, :], 1 + n) for n in range(layers)]
    up_copies = [load(up.at[n], up_raw.at[n], 1 + layers + n) for n in range(layers)]
    table_copy = load(table.at[0], table_half, pieces + 1)
    ids_copy = load(ids_hbm, ids, pieces + 2)
    bias_copy = load(bias, biases.at[m], pieces + 3)
    order_copy = load(order_hbm, order, pieces + 4)
    tower_bias_copy = load(tower_bias_hbm, tower_bias, pieces + 5)

    def lend(p):
        for k in STEPS:
            mine = slot(p, m, d)
            send(mine, mine, p % 2, z_recv.at[p, k - 1], d, goes(k))

    def spread(p, k):
        mine = slot(p, came(k), d)
        arrived(mine, z_recv.at[p, k - 1])
        send(mine, mine, p % 2, plane_recv.at[p, k - 1], chip_x * 2 + c, m)
        send(mine, mine, p % 2, plane_recv.at[p, k - 1], chip_y * 2 + c, m)
        send(mine, mine, p % 2, pair_recv.at[p, k - 1], partner, m)

    def relay(p, k):
        arrived(amount(p, 2), plane_recv.at[p, k - 1])
        for j in range(2):
            half = slot(p, came(k), chips[j] * 2 + c, j)
            send(half, half, p % 2, diag_recv.at[p, k - 1], chips[1 - j] * 2 + c, m)
        for j in range(2):
            whole = slot(p, came(k), chips[j] * 2 + c)
            send(whole, whole, p % 2, pair_recv.at[p, k - 1], partner, m)

    def corner(p, k):
        far = slot(p, came(k), chip_z * 2 + c)
        arrived(far, diag_recv.at[p, k - 1])
        send(far, far, p % 2, pair_recv.at[p, k - 1], partner, m)

    def complete(p, k):
        arrived(amount(p, CHIPS), pair_recv.at[p, k - 1])

    def tower_spread():
        mine = tower_slot(d)
        send(mine, mine, 2, tower_recv.at[0], chip_x * 2 + c, m)
        send(mine, mine, 2, tower_recv.at[0], chip_y * 2 + c, m)
        send(mine, mine, 2, tower_recv.at[2], partner, m)

    def tower_relay():
        arrived(tower_all.at[pl.ds(0, 2 * depth), :], tower_recv.at[0])
        for j in range(2):
            half = tower_slot(chips[j] * 2 + c, j)
            send(half, half, 2, tower_recv.at[1], chips[1 - j] * 2 + c, m)
        for j in range(2):
            whole = tower_slot(chips[j] * 2 + c)
            send(whole, whole, 2, tower_recv.at[2], partner, m)

    def tower_corner():
        far = tower_slot(chip_z * 2 + c)
        arrived(far, tower_recv.at[1])
        send(far, far, 2, tower_recv.at[2], partner, m)

    step = 16 if rows % 16 == 0 else 8

    def pool(group):
        first = pl.multiple_of((group * members + m) * rows, rows)

        def some(index, carry):
            base = pl.multiple_of(index * step, step)
            for r in range(step):
                total = None
                for hot in range(hots):
                    at = ids[hot, first + base + r]
                    row = table_wide[pl.ds(at, 1), :]
                    total = row if total is None else total + row
                sums[pl.ds(base + r, 1), :] = total
            return carry

        lax.fori_loop(0, rows // step, some, 0)
        return sums[...].astype(jnp.bfloat16)

    def pool_out(i):
        if i == 0:
            pooled[m, d] = pool(d)
        else:
            outbox[i] = pool(wrap(d + i, groups))

    def pool_away(i):
        send(outbox.at[i], pooled.at[m, d], 3, pool_recv.at[0], wrap(d + i, groups), m)

    half_of = lax.div(m, 2)
    beside = m + 1 - 2 * lax.rem(m, 2)
    across = 2 - half_of
    far_first = 2 * (1 - half_of)
    inner = jnp.logical_or(m == 1, m == 2)

    def share():
        arrived(outbox.at[pl.ds(0, groups - 1)], pool_recv.at[0])
        mine = pooled.at[m]
        send(mine, mine, 4, share_recv.at[m], d, across)
        send(mine, mine, 4, share_recv.at[m], d, beside)

    def pass_on(far):
        quarter = m + 2 - 4 * half_of if far else 3 - m

        @pl.when(inner)
        def _():
            theirs = pooled.at[quarter]
            arrived(theirs, share_recv.at[quarter])
            send(theirs, theirs, 4, share_recv.at[quarter], d, beside)

    def shared():
        arrived(pooled.at[beside], share_recv.at[beside])

        @pl.when(jnp.logical_not(inner))
        def _():
            for j in range(2):
                arrived(pooled.at[far_first + j], share_recv.at[far_first + j])

    def embed_all():
        per_block = block // embed
        order_copy.wait()
        for b in range(members):
            for f in range(per_block):
                at = order[b * per_block + f]
                for quarter in range(members):
                    embedded[
                        b, quarter * rows : (quarter + 1) * rows, f * embed : (f + 1) * embed
                    ] = pooled[quarter, at]

    def project(layer):
        state = embedded if layer == 0 else crossed
        value = None
        for b in range(members):
            term = jnp.dot(
                state[b],
                weights[layer, b * block : (b + 1) * block, :],
                preferred_element_type=jnp.float32,
            )
            value = term if value is None else value + term
        return value.astype(jnp.bfloat16)

    def lift(layer, projected, b):
        state = embedded if layer == 0 else crossed
        lifted = jnp.dot(projected, lifts[layer, b], preferred_element_type=jnp.float32)
        wide = embedded[b].astype(jnp.float32)
        value = wide * (lifted + biases[b, layer : layer + 1, :]) + state[b].astype(jnp.float32)
        return value.astype(jnp.bfloat16)

    order_of = tuple(range(0, pieces - 1, 2)) + tuple(range(1, pieces, 2))
    units = [(p, k) for p in order_of for k in STEPS]

    def do(call, *args):
        with jax.named_scope(call.__name__ + "_".join(map(str, args))):
            return call(*args)

    def first_sends():
        tower_copy.wait()
        for copy in weight_copies:
            copy.wait()
        bias_copy.wait()
        pl.semaphore_wait(barrier, members - 1 + groups - 1)
        tower_spread()
        lend(0)
        for k in range(1, members):
            send(biases.at[m], biases.at[m], 5, bias_recv.at[0], d, goes(k))
        lend(2)

    def flip():
        for n in range(layers):
            up_copies[n].wait()
            lifts[n, m] = up_raw[n].T

    def widen():
        table_copy.wait()
        table_wide[...] = table_half[...].astype(jnp.float32)
        ids_copy.wait()

    state = {}

    def ready():
        shared()
        embed_all()
        arrived(biases.at[pl.ds(0, others)], bias_recv.at[0])

    def narrow(layer):
        for k in STEPS:
            complete(2 * layer, k)
        state["projected"] = project(layer)

    def lift_first():
        for k in STEPS:
            complete(1, k)
        for b in range(members):
            crossed[b] = lift(0, state["projected"], b)

    def lift_last(*steps):
        for k in steps:
            if k:
                complete(pieces - 1, k)
            else:
                tower_bias_copy.wait()
                arrived(tower_all.at[pl.ds(0, CHIPS * depth), :], tower_recv.at[2])
        for k in steps:
            b = came(k)
            value = lift(layers - 1, state["projected"], b)
            part = jnp.dot(
                value,
                tower_all[pl.ds(pl.multiple_of(b * block, block), block), :],
                preferred_element_type=jnp.float32,
            )
            state["answer"] = state["answer"] + part if "answer" in state else part

    def finish():
        total = state["answer"] + tower_bias[...]
        out[...] = jnp.maximum(total, 0.0).astype(jnp.bfloat16)

    def sent(ref, which):
        remote(ref, ref, which, bias_recv.at[0], partner, m).wait_send()

    def all_sent():
        sent(weights.at[:, pl.ds(0, others * block), :], 0)
        sent(lifts.at[:, pl.ds(0, others)], 1)
        sent(tower_all.at[pl.ds(0, 7 * depth), :], 2)
        sent(outbox.at[pl.ds(0, groups - 1)], 3)
        sent(pooled.at[pl.ds(0, 2)], 4)

        @pl.when(inner)
        def _():
            sent(pooled.at[pl.ds(0, 2)], 4)

        sent(biases.at[pl.ds(0, others)], 5)

    calls = {
        "P": pool_out,
        "A": pool_away,
        "L": lend,
        "F": pass_on,
        "X": narrow,
    }
    on_units = {"S": spread, "R": relay, "C": corner}
    words = {
        "flip": flip,
        "widen": widen,
        "TR": tower_relay,
        "TC": tower_corner,
        "SH": share,
        "E": ready,
        "Y": lift_first,
        "end": finish,
    }
    do(first_sends)
    for word in PLAN:
        if word in words:
            do(words[word])
        elif word[0] in on_units:
            do(on_units[word[0]], *units[int(word[1:])])
        elif word[0] == "Z":
            do(lift_last, *map(int, word[1:]))
        else:
            do(calls[word[0]], int(word[1:]))
    do(all_sent)


def fused_body(
    feature_ids,
    tables,
    table_of_feature,
    cross_down,
    cross_up,
    cross_bias,
    tower_weight,
    tower_bias,
):
    groups = lax.axis_size("dp")
    members = lax.axis_size("mp")
    _, batch_size, hot_count = feature_ids.shape
    rows = batch_size // (groups * members)
    _, vocab, embed = tables.shape
    layers, block, rank = cross_down.shape
    depth, units = tower_weight.shape
    width = block * members
    pieces = 2 * layers
    dma = pltpu.SemaphoreType.DMA
    anywhere = pl.BlockSpec(memory_space=pl.ANY)
    vmem = pl.BlockSpec(memory_space=pltpu.VMEM)
    return pl.pallas_call(
        functools.partial(kernel, groups, members),
        out_shape=pltpu.VMEM((rows * members, units), jnp.bfloat16),
        in_specs=[anywhere] * 8,
        out_specs=vmem,
        scratch_shapes=[
            pltpu.SMEM((hot_count, batch_size), jnp.int32),
            pltpu.SMEM(table_of_feature.shape, jnp.int32),
            pltpu.VMEM((vocab, embed), jnp.bfloat16),
            pltpu.VMEM((vocab, embed), jnp.float32),
            pltpu.VMEM((rows, embed), jnp.float32),
            pltpu.VMEM((groups, rows, embed), jnp.bfloat16),
            pltpu.VMEM((members, groups, rows, embed), jnp.bfloat16),
            pltpu.VMEM((members, rows * members, block), jnp.bfloat16),
            pltpu.VMEM((members, rows * members, block), jnp.bfloat16),
            pltpu.VMEM((layers, width, rank), jnp.bfloat16),
            pltpu.VMEM((layers, block, rank), jnp.bfloat16),
            pltpu.VMEM((layers, members, rank, block), jnp.bfloat16),
            pltpu.VMEM((members, layers, block), jnp.float32),
            pltpu.VMEM((width, units), jnp.bfloat16),
            pltpu.VMEM((1, units), jnp.float32),
            dma((6 + pieces,)),
            dma((6,)),
            dma((pieces, members - 1)),
            dma((pieces, members - 1)),
            dma((pieces, members - 1)),
            dma((pieces, members - 1)),
            dma((3,)),
            dma((1,)),
            dma((members,)),
            dma((1,)),
        ],
        compiler_params=pltpu.CompilerParams(
            collective_id=0, has_side_effects=True, vmem_limit_bytes=VMEM_BYTES
        ),
    )(
        feature_ids[0].T,
        table_of_feature,
        tables,
        cross_down,
        cross_up,
        cross_bias,
        tower_weight,
        tower_bias.reshape(1, -1),
    )


def body(
    feature_ids,
    tables,
    table_of_feature,
    cross_down,
    cross_up,
    cross_bias,
    tower_weight,
    tower_bias,
):
    groups = lax.axis_size("dp")
    members = lax.axis_size("mp")
    held = 2 * members * (cross_down.size + cross_up.size) + 2 * groups * tower_weight.size
    placed = groups == 2 * CHIPS and members == PLANES
    fits = held <= KERNEL_BYTES and placed and tables.shape[0] == 1
    chosen = fused_body if fits else plain_body
    return chosen(
        feature_ids,
        tables,
        table_of_feature,
        cross_down,
        cross_up,
        cross_bias,
        tower_weight,
        tower_bias,
    )


def solution(mesh):
    return jax.shard_map(
        body,
        mesh=mesh,
        in_specs=(
            P("dp", None, None),
            P("dp", None, None),
            P(),
            P(None, "mp", None),
            P(None, "mp", None),
            P(None, "mp"),
            P("dp", "mp"),
            P("mp"),
        ),
        out_specs=P("dp", "mp"),
        check_vma=False,
    )
```

```python
import functools

import jax
import jax.numpy as jnp
from jax import lax
from jax.experimental import pallas as pl
from jax.experimental.pallas import tpu as pltpu
from jax.sharding import PartitionSpec as P


def plain_body(
    feature_ids,
    tables,
    table_of_feature,
    cross_down,
    cross_up,
    cross_bias,
    tower_weight,
    tower_bias,
):
    groups = lax.axis_size("dp")
    members = lax.axis_size("mp")
    member = lax.axis_index("mp")
    table_count, batch_size, hot_count = feature_ids.shape
    row_count = batch_size // (groups * members)
    shaped = feature_ids[0].reshape(groups, members, row_count, hot_count)
    own_ids = lax.dynamic_index_in_dim(shaped, member, 1, keepdims=False).reshape(
        groups * row_count, hot_count
    )
    summed = jnp.zeros((groups * row_count, tables.shape[2]), jnp.float32)
    for hot_index in range(hot_count):
        summed = summed + jnp.take(tables[0], own_ids[:, hot_index], axis=0).astype(jnp.float32)
    columns = [summed.astype(jnp.bfloat16)]
    pooled = jnp.stack(columns, axis=1)
    regrouped = lax.all_to_all(pooled, "dp", split_axis=0, concat_axis=1, tiled=True)
    ordered = jnp.take(regrouped, table_of_feature, axis=1)
    by_width = lax.all_to_all(ordered, "mp", split_axis=1, concat_axis=0, tiled=True)
    group_rows = by_width.shape[0]
    embedded = by_width.reshape(group_rows, -1)
    embedded_wide = embedded.astype(jnp.float32)
    crossed = embedded
    layer_total = cross_down.shape[0]
    for layer_index in range(layer_total):
        partial_value = jnp.dot(
            crossed, cross_down[layer_index], preferred_element_type=jnp.float32
        )
        projected = lax.psum(partial_value.astype(jnp.bfloat16), "mp")
        lifted = lax.dot_general(
            projected,
            cross_up[layer_index],
            (((1,), (1,)), ((), ())),
            preferred_element_type=jnp.float32,
        )
        crossed = (
            embedded_wide * (lifted + cross_bias[layer_index]) + crossed.astype(jnp.float32)
        ).astype(jnp.bfloat16)
    full_rows = lax.all_gather(crossed, "mp", axis=1, tiled=True)
    pre_act = jnp.dot(
        full_rows,
        lax.all_gather(tower_weight, "dp", axis=0, tiled=True),
        preferred_element_type=jnp.float32,
    )
    return jax.nn.relu(pre_act + tower_bias).astype(jnp.bfloat16)


MESH = pl.DeviceIdType.MESH
KERNEL_BYTES = 24 * 1024 * 1024
VMEM_BYTES = (64 * 1024 - 352) * 1024
CHIPS = 4
PLANES = 4
LANES = 128
STEPS = (1, 3, 2)
PLAN = (
    "flip", "widen", "P1", "L1", "L3", "P2", "A1", "P3", "A2", "P4", "A3", "P5", "A4", "P6",
    "A5", "P7", "A6", "P0", "A7", "S0", "S1", "TR", "S2", "S3", "HA", "S4", "S5", "S6", "S7",
    "R0", "S8", "S9", "R1", "S10", "R2", "S11", "HB", "F1", "R3", "R4", "R5", "F0", "C0", "C1",
    "C2", "TC", "R6", "R7", "R8", "C3", "C4", "C5", "R9", "R10", "R11", "C6", "C7", "C8", "E",
    "X0", "Y", "C9", "C10", "C11", "X1", "Z01", "Z32", "end",
)


def kernel(
    groups,
    members,
    ids_hbm,
    order_hbm,
    table,
    down,
    up,
    bias,
    tower,
    tower_bias_hbm,
    out,
    ids,
    order,
    table_half,
    table_wide,
    sums,
    outbox,
    pooled,
    embedded,
    crossed,
    weights,
    up_raw,
    lifts,
    biases,
    tower_all,
    tower_bias,
    local_sem,
    send_sem,
    z_recv,
    plane_recv,
    diag_recv,
    pair_recv,
    tower_recv,
    pool_recv,
    share_recv,
    bias_recv,
):
    d = lax.axis_index("dp")
    m = lax.axis_index("mp")
    q = lax.div(d, 2)
    c = lax.rem(d, 2)
    partner = q * 2 + 1 - c
    chip_x = q + 1 - 2 * lax.rem(q, 2)
    chip_y = lax.rem(q + 2, CHIPS)
    chip_z = lax.rem(chip_x + 2, CHIPS)
    chips = (chip_x, chip_y, chip_z)
    layers, block, rank = down.shape
    rows, embed = sums.shape
    hots = ids.shape[0] // (rows * groups * members)
    piece = block // groups
    depth = tower.shape[0]
    pieces = 2 * layers
    others = members - 1

    def wrap(value, size):
        return lax.rem(value + size, size)

    def load(src, dst, index):
        copy = pltpu.make_async_copy(src, dst, local_sem.at[index])
        copy.start()
        return copy

    def remote(src, dst, which, recv_sem, to_d, to_m):
        return pltpu.make_async_remote_copy(
            src_ref=src,
            dst_ref=dst,
            send_sem=send_sem.at[which],
            recv_sem=recv_sem,
            device_id=(to_d, to_m),
            device_id_type=MESH,
        )

    def send(src, dst, which, recv_sem, to_d, to_m):
        remote(src, dst, which, recv_sem, to_d, to_m).start()

    def arrived(ref, recv_sem):
        remote(ref, ref, 0, recv_sem, partner, m).wait_recv()

    half_of = lax.div(m, 2)
    beside = m + 1 - 2 * lax.rem(m, 2)
    across = 2 - half_of
    far_first = 2 * (1 - half_of)
    inner = jnp.logical_or(m == 1, m == 2)
    outermost = 3 * (1 - half_of)

    def came(k):
        return (m, beside, across, outermost)[k]

    def goes(k):
        return wrap(m + k, members)

    thin = rank // groups

    def slot(p, member, device, half=None):
        full = piece if p % 2 == 0 else thin
        length = full if half is None else full // 2
        start = device * full + (0 if half is None else half * length)
        if p % 2 == 0:
            start = member * block + start
            return weights.at[p // 2, pl.ds(pl.multiple_of(start, length), length), :]
        return lifts.at[p // 2, member, pl.ds(pl.multiple_of(start, length), length), :]

    def amount(p, count):
        if p % 2 == 0:
            return weights.at[p // 2, pl.ds(0, count * piece), :]
        return lifts.at[p // 2, 0, pl.ds(0, count * thin), :]

    def tower_slot(device, half=None):
        length = depth if half is None else depth // 2
        start = device * depth + (0 if half is None else half * length)
        return tower_all.at[pl.ds(pl.multiple_of(start, length), length), :]

    barrier = pltpu.get_barrier_semaphore()
    for k in range(1, members):
        pl.semaphore_signal(barrier, inc=1, device_id=(d, goes(k)), device_id_type=MESH)
    for i in range(1, groups):
        pl.semaphore_signal(barrier, inc=1, device_id=(wrap(d + i, groups), m), device_id_type=MESH)

    here = pl.ds(pl.multiple_of(m * block, block), block)
    tower_copy = load(tower, tower_slot(d), 0)
    weight_copies = [load(down.at[n], weights.at[n, here, :], 1 + n) for n in range(layers)]
    up_copies = [load(up.at[n], up_raw.at[n], 1 + layers + n) for n in range(layers)]
    table_copy = load(table.at[0], table_half, pieces + 1)
    ids_copy = load(ids_hbm, ids, pieces + 2)
    bias_copy = load(bias, biases.at[m], pieces + 3)
    order_copy = load(order_hbm, order, pieces + 4)
    tower_bias_copy = load(tower_bias_hbm, tower_bias, pieces + 5)

    place = 3 - lax.rem(m + half_of, 2)

    def lend(p):
        mine = slot(p, m, d)
        send(mine, mine, p % 2, z_recv.at[p, place - 1], d, across)
        send(mine, mine, p % 2, z_recv.at[p, 0], d, beside)

    def spread(p, k):
        mine = slot(p, came(k), d)
        arrived(mine, z_recv.at[p, k - 1])
        if k > 1:

            @pl.when(inner)
            def _():
                send(mine, mine, p % 2, z_recv.at[p, k - 1], d, beside)

        send(mine, mine, p % 2, plane_recv.at[p, k - 1], chip_x * 2 + c, m)
        send(mine, mine, p % 2, plane_recv.at[p, k - 1], chip_y * 2 + c, m)
        send(mine, mine, p % 2, pair_recv.at[p, k - 1], partner, m)

    def relay(p, k):
        arrived(amount(p, 2), plane_recv.at[p, k - 1])
        for j in range(2):
            half = slot(p, came(k), chips[j] * 2 + c, j)
            send(half, half, p % 2, diag_recv.at[p, k - 1], chips[1 - j] * 2 + c, m)
        for j in range(2):
            whole = slot(p, came(k), chips[j] * 2 + c)
            send(whole, whole, p % 2, pair_recv.at[p, k - 1], partner, m)

    def corner(p, k):
        far = slot(p, came(k), chip_z * 2 + c)
        arrived(far, diag_recv.at[p, k - 1])
        send(far, far, p % 2, pair_recv.at[p, k - 1], partner, m)

    def complete(p, k):
        arrived(amount(p, CHIPS), pair_recv.at[p, k - 1])

    def tower_spread():
        mine = tower_slot(d)
        send(mine, mine, 2, tower_recv.at[0], chip_x * 2 + c, m)
        send(mine, mine, 2, tower_recv.at[0], chip_y * 2 + c, m)
        send(mine, mine, 2, tower_recv.at[2], partner, m)

    def tower_relay():
        arrived(tower_all.at[pl.ds(0, 2 * depth), :], tower_recv.at[0])
        for j in range(2):
            half = tower_slot(chips[j] * 2 + c, j)
            send(half, half, 2, tower_recv.at[1], chips[1 - j] * 2 + c, m)
        for j in range(2):
            whole = tower_slot(chips[j] * 2 + c)
            send(whole, whole, 2, tower_recv.at[2], partner, m)

    def tower_corner():
        far = tower_slot(chip_z * 2 + c)
        arrived(far, tower_recv.at[1])
        send(far, far, 2, tower_recv.at[2], partner, m)

    step = 16 if rows % 16 == 0 else 8

    def pool(group):
        first = (group * members + m) * rows

        def some(index, carry):
            base = pl.multiple_of(index * step, step)
            lane = first + base
            word = lax.div(lane, LANES) * (LANES * hots) + lax.rem(lane, LANES)
            for r in range(step):
                total = None
                for hot in range(hots):
                    at = ids[word + (hot * LANES + r)]
                    row = table_wide[pl.ds(at, 1), :]
                    total = row if total is None else total + row
                sums[pl.ds(base + r, 1), :] = total
            return carry

        lax.fori_loop(0, rows // step, some, 0)
        return sums[...].astype(jnp.bfloat16)

    def pool_out(i):
        if i == 0:
            pooled[m, d] = pool(d)
        else:
            outbox[i] = pool(wrap(d + i, groups))

    def pool_away(i):
        send(outbox.at[i], pooled.at[m, d], 3, pool_recv.at[0], wrap(d + i, groups), m)

    def share_across():
        arrived(outbox.at[pl.ds(0, groups - 1)], pool_recv.at[0])
        send(pooled.at[m], pooled.at[m], 4, share_recv.at[m], d, across)

    def share_beside():
        send(pooled.at[m], pooled.at[m], 4, share_recv.at[m], d, beside)

    def pass_on(far):
        quarter = m + 2 - 4 * half_of if far else 3 - m

        @pl.when(inner)
        def _():
            theirs = pooled.at[quarter]
            arrived(theirs, share_recv.at[quarter])
            send(theirs, theirs, 4, share_recv.at[quarter], d, beside)

    def shared():
        arrived(pooled.at[beside], share_recv.at[beside])

        @pl.when(jnp.logical_not(inner))
        def _():
            for j in range(2):
                arrived(pooled.at[far_first + j], share_recv.at[far_first + j])

    def embed_all():
        per_block = block // embed
        order_copy.wait()
        for b in range(members):
            for f in range(per_block):
                at = order[b * per_block + f]
                for quarter in range(members):
                    embedded[
                        b, quarter * rows : (quarter + 1) * rows, f * embed : (f + 1) * embed
                    ] = pooled[quarter, at]

    def project(layer):
        state = embedded if layer == 0 else crossed
        value = None
        for b in range(members):
            term = jnp.dot(
                state[b],
                weights[layer, b * block : (b + 1) * block, :],
                preferred_element_type=jnp.float32,
            )
            value = term if value is None else value + term
        return value.astype(jnp.bfloat16)

    def lift(layer, projected, b):
        state = embedded if layer == 0 else crossed
        lifted = jnp.dot(projected, lifts[layer, b], preferred_element_type=jnp.float32)
        wide = embedded[b].astype(jnp.float32)
        value = wide * (lifted + biases[b, layer : layer + 1, :]) + state[b].astype(jnp.float32)
        return value.astype(jnp.bfloat16)

    order_of = tuple(range(0, pieces - 1, 2)) + tuple(range(1, pieces, 2))
    units = [(p, k) for p in order_of for k in STEPS]

    def do(call, *args):
        with jax.named_scope(call.__name__ + "_".join(map(str, args))):
            return call(*args)

    def first_sends():
        tower_copy.wait()
        for copy in weight_copies:
            copy.wait()
        bias_copy.wait()
        pl.semaphore_wait(barrier, members - 1 + groups - 1)
        tower_spread()
        lend(0)
        for k in range(1, members):
            send(biases.at[m], biases.at[m], 5, bias_recv.at[0], d, goes(k))
        lend(2)

    def flip():
        for n in range(layers):
            up_copies[n].wait()
            lifts[n, m] = up_raw[n].T

    def widen():
        table_copy.wait()
        table_wide[...] = table_half[...].astype(jnp.float32)
        ids_copy.wait()

    state = {}

    def ready():
        shared()
        embed_all()
        arrived(biases.at[pl.ds(0, others)], bias_recv.at[0])

    def narrow(layer):
        for k in STEPS:
            complete(2 * layer, k)
        state["projected"] = project(layer)

    def lift_first():
        for k in STEPS:
            complete(1, k)
        for b in range(members):
            crossed[b] = lift(0, state["projected"], b)

    def lift_last(*steps):
        for k in steps:
            if k:
                complete(pieces - 1, k)
            else:
                tower_bias_copy.wait()
                arrived(tower_all.at[pl.ds(0, CHIPS * depth), :], tower_recv.at[2])
        for k in steps:
            b = came(k)
            value = lift(layers - 1, state["projected"], b)
            part = jnp.dot(
                value,
                tower_all[pl.ds(pl.multiple_of(b * block, block), block), :],
                preferred_element_type=jnp.float32,
            )
            state["answer"] = state["answer"] + part if "answer" in state else part

    def finish():
        total = state["answer"] + tower_bias[...]
        out[...] = jnp.maximum(total, 0.0).astype(jnp.bfloat16)

    def sent(ref, which):
        remote(ref, ref, which, bias_recv.at[0], partner, m).wait_send()

    def all_sent():
        total = others * (groups - 1) + 2
        sent(weights.at[:, pl.ds(0, total * piece), :], 0)
        sent(weights.at[:, pl.ds(0, total * piece), :], 1)
        sent(tower_all.at[pl.ds(0, 7 * depth), :], 2)
        sent(outbox.at[pl.ds(0, groups - 1)], 3)
        sent(pooled.at[pl.ds(0, 2)], 4)

        @pl.when(inner)
        def _():
            sent(weights.at[:, pl.ds(0, 2 * piece), :], 0)
            sent(weights.at[:, pl.ds(0, 2 * piece), :], 1)
            sent(pooled.at[pl.ds(0, 2)], 4)

        sent(biases.at[pl.ds(0, others)], 5)

    calls = {
        "P": pool_out,
        "A": pool_away,
        "L": lend,
        "F": pass_on,
        "X": narrow,
    }
    on_units = {"S": spread, "R": relay, "C": corner}
    words = {
        "flip": flip,
        "widen": widen,
        "TR": tower_relay,
        "TC": tower_corner,
        "HA": share_across,
        "HB": share_beside,
        "E": ready,
        "Y": lift_first,
        "end": finish,
    }
    do(first_sends)
    for word in PLAN:
        if word in words:
            do(words[word])
        elif word[0] in on_units:
            do(on_units[word[0]], *units[int(word[1:])])
        elif word[0] == "Z":
            do(lift_last, *map(int, word[1:]))
        else:
            do(calls[word[0]], int(word[1:]))
    do(all_sent)


def fused_body(
    feature_ids,
    tables,
    table_of_feature,
    cross_down,
    cross_up,
    cross_bias,
    tower_weight,
    tower_bias,
):
    groups = lax.axis_size("dp")
    members = lax.axis_size("mp")
    _, batch_size, hot_count = feature_ids.shape
    rows = batch_size // (groups * members)
    _, vocab, embed = tables.shape
    layers, block, rank = cross_down.shape
    depth, units = tower_weight.shape
    width = block * members
    pieces = 2 * layers
    dma = pltpu.SemaphoreType.DMA
    anywhere = pl.BlockSpec(memory_space=pl.ANY)
    vmem = pl.BlockSpec(memory_space=pltpu.VMEM)
    return pl.pallas_call(
        functools.partial(kernel, groups, members),
        out_shape=pltpu.VMEM((rows * members, units), jnp.bfloat16),
        in_specs=[anywhere] * 8,
        out_specs=vmem,
        scratch_shapes=[
            pltpu.SMEM((hot_count * batch_size,), jnp.int32),
            pltpu.SMEM(table_of_feature.shape, jnp.int32),
            pltpu.VMEM((vocab, embed), jnp.bfloat16),
            pltpu.VMEM((vocab, embed), jnp.float32),
            pltpu.VMEM((rows, embed), jnp.float32),
            pltpu.VMEM((groups, rows, embed), jnp.bfloat16),
            pltpu.VMEM((members, groups, rows, embed), jnp.bfloat16),
            pltpu.VMEM((members, rows * members, block), jnp.bfloat16),
            pltpu.VMEM((members, rows * members, block), jnp.bfloat16),
            pltpu.VMEM((layers, width, rank), jnp.bfloat16),
            pltpu.VMEM((layers, block, rank), jnp.bfloat16),
            pltpu.VMEM((layers, members, rank, block), jnp.bfloat16),
            pltpu.VMEM((members, layers, block), jnp.float32),
            pltpu.VMEM((width, units), jnp.bfloat16),
            pltpu.VMEM((1, units), jnp.float32),
            dma((6 + pieces,)),
            dma((6,)),
            dma((pieces, members - 1)),
            dma((pieces, members - 1)),
            dma((pieces, members - 1)),
            dma((pieces, members - 1)),
            dma((3,)),
            dma((1,)),
            dma((members,)),
            dma((1,)),
        ],
        compiler_params=pltpu.CompilerParams(
            collective_id=0, has_side_effects=True, vmem_limit_bytes=VMEM_BYTES
        ),
    )(
        feature_ids[0].reshape(-1, LANES, hot_count).transpose(0, 2, 1).reshape(-1),
        table_of_feature,
        tables,
        cross_down,
        cross_up,
        cross_bias,
        tower_weight,
        tower_bias.reshape(1, -1),
    )


def body(
    feature_ids,
    tables,
    table_of_feature,
    cross_down,
    cross_up,
    cross_bias,
    tower_weight,
    tower_bias,
):
    groups = lax.axis_size("dp")
    members = lax.axis_size("mp")
    held = 2 * members * (cross_down.size + cross_up.size) + 2 * groups * tower_weight.size
    placed = groups == 2 * CHIPS and members == PLANES
    even = feature_ids.shape[1] % LANES == 0
    fits = held <= KERNEL_BYTES and placed and even and tables.shape[0] == 1
    chosen = fused_body if fits else plain_body
    return chosen(
        feature_ids,
        tables,
        table_of_feature,
        cross_down,
        cross_up,
        cross_bias,
        tower_weight,
        tower_bias,
    )


def solution(mesh):
    return jax.shard_map(
        body,
        mesh=mesh,
        in_specs=(
            P("dp", None, None),
            P("dp", None, None),
            P(),
            P(None, "mp", None),
            P(None, "mp", None),
            P(None, "mp"),
            P("dp", "mp"),
            P("mp"),
        ),
        out_specs=P("dp", "mp"),
        check_vma=False,
    )
```

```python
import functools

import jax
import jax.numpy as jnp
from jax import lax
from jax.experimental import pallas as pl
from jax.experimental.pallas import tpu as pltpu
from jax.sharding import PartitionSpec as P


def plain_body(
    feature_ids,
    tables,
    table_of_feature,
    cross_down,
    cross_up,
    cross_bias,
    tower_weight,
    tower_bias,
):
    groups = lax.axis_size("dp")
    members = lax.axis_size("mp")
    member = lax.axis_index("mp")
    table_count, batch_size, hot_count = feature_ids.shape
    row_count = batch_size // (groups * members)
    shaped = feature_ids[0].reshape(groups, members, row_count, hot_count)
    own_ids = lax.dynamic_index_in_dim(shaped, member, 1, keepdims=False).reshape(
        groups * row_count, hot_count
    )
    summed = jnp.zeros((groups * row_count, tables.shape[2]), jnp.float32)
    for hot_index in range(hot_count):
        summed = summed + jnp.take(tables[0], own_ids[:, hot_index], axis=0).astype(jnp.float32)
    columns = [summed.astype(jnp.bfloat16)]
    pooled = jnp.stack(columns, axis=1)
    regrouped = lax.all_to_all(pooled, "dp", split_axis=0, concat_axis=1, tiled=True)
    ordered = jnp.take(regrouped, table_of_feature, axis=1)
    by_width = lax.all_to_all(ordered, "mp", split_axis=1, concat_axis=0, tiled=True)
    group_rows = by_width.shape[0]
    embedded = by_width.reshape(group_rows, -1)
    embedded_wide = embedded.astype(jnp.float32)
    crossed = embedded
    layer_total = cross_down.shape[0]
    for layer_index in range(layer_total):
        partial_value = jnp.dot(
            crossed, cross_down[layer_index], preferred_element_type=jnp.float32
        )
        projected = lax.psum(partial_value.astype(jnp.bfloat16), "mp")
        lifted = lax.dot_general(
            projected,
            cross_up[layer_index],
            (((1,), (1,)), ((), ())),
            preferred_element_type=jnp.float32,
        )
        crossed = (
            embedded_wide * (lifted + cross_bias[layer_index]) + crossed.astype(jnp.float32)
        ).astype(jnp.bfloat16)
    full_rows = lax.all_gather(crossed, "mp", axis=1, tiled=True)
    pre_act = jnp.dot(
        full_rows,
        lax.all_gather(tower_weight, "dp", axis=0, tiled=True),
        preferred_element_type=jnp.float32,
    )
    return jax.nn.relu(pre_act + tower_bias).astype(jnp.bfloat16)


MESH = pl.DeviceIdType.MESH
KERNEL_BYTES = 24 * 1024 * 1024
VMEM_BYTES = (64 * 1024 - 352) * 1024
CHIPS = 4
PLANES = 4
LANES = 128
STEPS = (1, 3, 2)
FIRST = (
    "flip", "widen", "P1", "L1", "L2", "L3", "P2", "A1", "P3", "A2", "P4", "A3", "P5", "A4",
    "P6", "A5", "P7", "A6", "P0", "A7",
)
INNER = (
    "S0", "T1", "T2", "S3", "T4", "T5", "R0", "S6", "T7", "T8", "HA", "S9", "T10", "T11", "HB",
    "R1", "R2", "R3", "R4", "R5", "F1", "R6", "R7", "R8", "R9", "F0", "R10", "R11", "WR", "C0",
    "C1", "C2", "C3", "C4", "C5",
)
OUTER = (
    "S0", "S3", "S6", "S9", "HA", "HB", "S1", "S2", "R0", "S4", "S5", "R3", "S7", "S8", "R6",
    "S10", "S11", "R9", "R1", "R2", "R4", "R5", "R7", "R8", "R10", "R11", "C0", "C3", "WR",
    "C1", "C2", "C4", "C5",
)
LAST = (
    "C6", "C7", "C8", "E", "X0", "C9", "C10", "C11", "WC", "Y", "X1", "Z", "end",
)


def kernel(
    groups,
    members,
    ids_hbm,
    order_hbm,
    table,
    down,
    up,
    bias,
    tower,
    tower_bias_hbm,
    out,
    ids,
    order,
    table_half,
    table_wide,
    sums,
    outbox,
    pooled,
    embedded,
    crossed,
    weights,
    up_raw,
    lifts,
    biases,
    tower_all,
    tower_bias,
    local_sem,
    send_sem,
    z_recv,
    plane_recv,
    diag_recv,
    pair_recv,
    tower_recv,
    pool_recv,
    share_recv,
    bias_recv,
):
    d = lax.axis_index("dp")
    m = lax.axis_index("mp")
    q = lax.div(d, 2)
    c = lax.rem(d, 2)
    partner = q * 2 + 1 - c
    chip_x = q + 1 - 2 * lax.rem(q, 2)
    chip_y = lax.rem(q + 2, CHIPS)
    chip_z = lax.rem(chip_x + 2, CHIPS)
    chips = (chip_x, chip_y, chip_z)
    layers, block, rank = down.shape
    rows, embed = sums.shape
    hots = ids.shape[0] // (rows * groups * members)
    piece = block // groups
    depth = tower.shape[0]
    pieces = 2 * layers
    others = members - 1

    def wrap(value, size):
        return lax.rem(value + size, size)

    def load(src, dst, index):
        copy = pltpu.make_async_copy(src, dst, local_sem.at[index])
        copy.start()
        return copy

    def remote(src, dst, which, recv_sem, to_d, to_m):
        return pltpu.make_async_remote_copy(
            src_ref=src,
            dst_ref=dst,
            send_sem=send_sem.at[which],
            recv_sem=recv_sem,
            device_id=(to_d, to_m),
            device_id_type=MESH,
        )

    def send(src, dst, which, recv_sem, to_d, to_m):
        remote(src, dst, which, recv_sem, to_d, to_m).start()

    def arrived(ref, recv_sem):
        remote(ref, ref, 0, recv_sem, partner, m).wait_recv()

    half_of = lax.div(m, 2)
    beside = m + 1 - 2 * lax.rem(m, 2)
    across = 2 - half_of
    far_first = 2 * (1 - half_of)
    inner = jnp.logical_or(m == 1, m == 2)
    outermost = 3 * (1 - half_of)

    def came(k):
        return (m, beside, across, outermost)[k]

    def goes(k):
        return wrap(m + k, members)

    thin = rank // groups

    def slot(p, member, device, half=None):
        full = piece if p % 2 == 0 else thin
        length = full if half is None else full // 2
        start = device * full + (0 if half is None else half * length)
        if p % 2 == 0:
            start = member * block + start
            return weights.at[p // 2, pl.ds(pl.multiple_of(start, length), length), :]
        return lifts.at[p // 2, member, pl.ds(pl.multiple_of(start, length), length), :]

    def amount(p, count):
        if p % 2 == 0:
            return weights.at[p // 2, pl.ds(0, count * piece), :]
        return lifts.at[p // 2, 0, pl.ds(0, count * thin), :]

    def tower_slot(device, half=None):
        length = depth if half is None else depth // 2
        start = device * depth + (0 if half is None else half * length)
        return tower_all.at[pl.ds(pl.multiple_of(start, length), length), :]

    barrier = pltpu.get_barrier_semaphore()
    for k in range(1, members):
        pl.semaphore_signal(barrier, inc=1, device_id=(d, goes(k)), device_id_type=MESH)
    for i in range(1, groups):
        pl.semaphore_signal(barrier, inc=1, device_id=(wrap(d + i, groups), m), device_id_type=MESH)

    here = pl.ds(pl.multiple_of(m * block, block), block)
    tower_copy = load(tower, tower_slot(d), 0)
    weight_copies = [load(down.at[n], weights.at[n, here, :], 1 + n) for n in range(layers)]
    up_copies = [load(up.at[n], up_raw.at[n], 1 + layers + n) for n in range(layers)]
    table_copy = load(table.at[0], table_half, pieces + 1)
    ids_copy = load(ids_hbm, ids, pieces + 2)
    bias_copy = load(bias, biases.at[m], pieces + 3)
    order_copy = load(order_hbm, order, pieces + 4)
    tower_bias_copy = load(tower_bias_hbm, tower_bias, pieces + 5)

    place = 3 - lax.rem(m + half_of, 2)

    def lend(p):
        mine = slot(p, m, d)
        send(mine, mine, p % 2, z_recv.at[p, place - 1], d, across)
        send(mine, mine, p % 2, z_recv.at[p, 0], d, beside)

    def spread(p, k):
        mine = slot(p, came(k), d)
        arrived(mine, z_recv.at[p, k - 1])
        send(mine, mine, p % 2, plane_recv.at[p, k - 1], chip_x * 2 + c, m)
        send(mine, mine, p % 2, plane_recv.at[p, k - 1], chip_y * 2 + c, m)
        send(mine, mine, p % 2, pair_recv.at[p, k - 1], partner, m)

    def pass_and_spread(p, k):
        mine = slot(p, came(k), d)
        arrived(mine, z_recv.at[p, k - 1])
        send(mine, mine, p % 2, z_recv.at[p, k - 1], d, beside)
        send(mine, mine, p % 2, plane_recv.at[p, k - 1], chip_x * 2 + c, m)
        send(mine, mine, p % 2, plane_recv.at[p, k - 1], chip_y * 2 + c, m)
        send(mine, mine, p % 2, pair_recv.at[p, k - 1], partner, m)

    def relay(p, k):
        arrived(amount(p, 2), plane_recv.at[p, k - 1])
        for j in range(2):
            half = slot(p, came(k), chips[j] * 2 + c, j)
            send(half, half, p % 2, diag_recv.at[p, k - 1], chips[1 - j] * 2 + c, m)
        for j in range(2):
            whole = slot(p, came(k), chips[j] * 2 + c)
            send(whole, whole, p % 2, pair_recv.at[p, k - 1], partner, m)

    def corner(p, k):
        far = slot(p, came(k), chip_z * 2 + c)
        arrived(far, diag_recv.at[p, k - 1])
        send(far, far, p % 2, pair_recv.at[p, k - 1], partner, m)

    def complete(p, k):
        arrived(amount(p, CHIPS), pair_recv.at[p, k - 1])

    def tower_spread():
        mine = tower_slot(d)
        send(mine, mine, 2, tower_recv.at[0], chip_x * 2 + c, m)
        send(mine, mine, 2, tower_recv.at[0], chip_y * 2 + c, m)
        send(mine, mine, 2, tower_recv.at[2], partner, m)

    def tower_relay():
        arrived(tower_all.at[pl.ds(0, 2 * depth), :], tower_recv.at[0])
        for j in range(2):
            half = tower_slot(chips[j] * 2 + c, j)
            send(half, half, 2, tower_recv.at[1], chips[1 - j] * 2 + c, m)
        for j in range(2):
            whole = tower_slot(chips[j] * 2 + c)
            send(whole, whole, 2, tower_recv.at[2], partner, m)

    def tower_corner():
        far = tower_slot(chip_z * 2 + c)
        arrived(far, tower_recv.at[1])
        send(far, far, 2, tower_recv.at[2], partner, m)

    step = 16 if rows % 16 == 0 else 8

    def pool(group):
        first = (group * members + m) * rows

        def some(index, carry):
            base = pl.multiple_of(index * step, step)
            lane = first + base
            word = lax.div(lane, LANES) * (LANES * hots) + lax.rem(lane, LANES)
            for r in range(step):
                total = None
                for hot in range(hots):
                    at = ids[word + (hot * LANES + r)]
                    row = table_wide[pl.ds(at, 1), :]
                    total = row if total is None else total + row
                sums[pl.ds(base + r, 1), :] = total
            return carry

        lax.fori_loop(0, rows // step, some, 0)
        return sums[...].astype(jnp.bfloat16)

    def pool_out(i):
        if i == 0:
            pooled[m, d] = pool(d)
        else:
            outbox[i] = pool(wrap(d + i, groups))

    def pool_away(i):
        send(outbox.at[i], pooled.at[m, d], 3, pool_recv.at[0], wrap(d + i, groups), m)

    def share_across():
        arrived(outbox.at[pl.ds(0, groups - 1)], pool_recv.at[0])
        send(pooled.at[m], pooled.at[m], 4, share_recv.at[m], d, across)

    def share_beside():
        send(pooled.at[m], pooled.at[m], 4, share_recv.at[m], d, beside)

    def pass_on(far):
        quarter = m + 2 - 4 * half_of if far else 3 - m
        theirs = pooled.at[quarter]
        arrived(theirs, share_recv.at[quarter])
        send(theirs, theirs, 4, share_recv.at[quarter], d, beside)

    def shared():
        arrived(pooled.at[beside], share_recv.at[beside])

        @pl.when(jnp.logical_not(inner))
        def _():
            for j in range(2):
                arrived(pooled.at[far_first + j], share_recv.at[far_first + j])

    def embed_all():
        per_block = block // embed
        order_copy.wait()
        for b in range(members):
            for f in range(per_block):
                at = order[b * per_block + f]
                for quarter in range(members):
                    embedded[
                        b, quarter * rows : (quarter + 1) * rows, f * embed : (f + 1) * embed
                    ] = pooled[quarter, at]

    def project(layer):
        state = embedded if layer == 0 else crossed
        value = None
        for b in range(members):
            term = jnp.dot(
                state[b],
                weights[layer, b * block : (b + 1) * block, :],
                preferred_element_type=jnp.float32,
            )
            value = term if value is None else value + term
        return value.astype(jnp.bfloat16)

    def lift(layer, projected, b):
        state = embedded if layer == 0 else crossed
        lifted = jnp.dot(projected, lifts[layer, b], preferred_element_type=jnp.float32)
        wide = embedded[b].astype(jnp.float32)
        value = wide * (lifted + biases[b, layer : layer + 1, :]) + state[b].astype(jnp.float32)
        return value.astype(jnp.bfloat16)

    units = [(p, k) for p in range(pieces) for k in STEPS]

    def do(call, *args):
        with jax.named_scope(call.__name__ + "_".join(map(str, args))):
            return call(*args)

    def first_sends():
        tower_copy.wait()
        pl.semaphore_wait(barrier, members - 1 + groups - 1)
        tower_spread()
        weight_copies[0].wait()
        lend(0)
        bias_copy.wait()
        for k in range(1, members):
            send(biases.at[m], biases.at[m], 5, bias_recv.at[0], d, goes(k))
        for copy in weight_copies[1:]:
            copy.wait()

    def flip():
        for n in range(layers):
            up_copies[n].wait()
            lifts[n, m] = up_raw[n].T

    def widen():
        table_copy.wait()
        table_wide[...] = table_half[...].astype(jnp.float32)
        ids_copy.wait()

    state = {}

    def ready():
        shared()
        embed_all()
        arrived(biases.at[pl.ds(0, others)], bias_recv.at[0])

    def narrow(layer):
        for k in STEPS:
            complete(2 * layer, k)
        state["projected"] = project(layer)

    def lift_first():
        for k in STEPS:
            complete(1, k)
        for b in range(members):
            crossed[b] = lift(0, state["projected"], b)

    def lift_last():
        for k in STEPS:
            complete(pieces - 1, k)
        for b in range(members):
            crossed[b] = lift(layers - 1, state["projected"], b)

    def finish():
        tower_bias_copy.wait()
        arrived(tower_all.at[pl.ds(0, CHIPS * depth), :], tower_recv.at[2])
        total = None
        for b in range(members):
            part = jnp.dot(
                crossed[b],
                tower_all[b * block : (b + 1) * block, :],
                preferred_element_type=jnp.float32,
            )
            total = part if total is None else total + part
        out[...] = jnp.maximum(total + tower_bias[...], 0.0).astype(jnp.bfloat16)

    def sent(ref, which):
        remote(ref, ref, which, bias_recv.at[0], partner, m).wait_send()

    def all_sent():
        total = others * (groups - 1) + 2
        sent(weights.at[:, pl.ds(0, total * piece), :], 0)
        sent(weights.at[:, pl.ds(0, total * piece), :], 1)
        sent(tower_all.at[pl.ds(0, 7 * depth), :], 2)
        sent(outbox.at[pl.ds(0, groups - 1)], 3)
        sent(pooled.at[pl.ds(0, 2)], 4)

        @pl.when(inner)
        def _():
            sent(weights.at[:, pl.ds(0, 2 * piece), :], 0)
            sent(weights.at[:, pl.ds(0, 2 * piece), :], 1)
            sent(pooled.at[pl.ds(0, 2)], 4)

        sent(biases.at[pl.ds(0, others)], 5)

    calls = {
        "P": pool_out,
        "A": pool_away,
        "L": lend,
        "F": pass_on,
        "X": narrow,
    }
    on_units = {"S": spread, "T": pass_and_spread, "R": relay, "C": corner}
    words = {
        "flip": flip,
        "widen": widen,
        "WR": tower_relay,
        "WC": tower_corner,
        "HA": share_across,
        "HB": share_beside,
        "E": ready,
        "Y": lift_first,
        "Z": lift_last,
        "end": finish,
    }
    def follow(plan):
        for word in plan:
            if word in words:
                do(words[word])
            elif word[0] in on_units:
                do(on_units[word[0]], *units[int(word[1:])])
            else:
                do(calls[word[0]], int(word[1:]))

    do(first_sends)
    follow(FIRST)

    @pl.when(inner)
    def _():
        follow(INNER)

    @pl.when(jnp.logical_not(inner))
    def _():
        follow(OUTER)

    follow(LAST)
    do(all_sent)


def fused_body(
    feature_ids,
    tables,
    table_of_feature,
    cross_down,
    cross_up,
    cross_bias,
    tower_weight,
    tower_bias,
):
    groups = lax.axis_size("dp")
    members = lax.axis_size("mp")
    _, batch_size, hot_count = feature_ids.shape
    rows = batch_size // (groups * members)
    _, vocab, embed = tables.shape
    layers, block, rank = cross_down.shape
    depth, units = tower_weight.shape
    width = block * members
    pieces = 2 * layers
    dma = pltpu.SemaphoreType.DMA
    anywhere = pl.BlockSpec(memory_space=pl.ANY)
    vmem = pl.BlockSpec(memory_space=pltpu.VMEM)
    return pl.pallas_call(
        functools.partial(kernel, groups, members),
        out_shape=pltpu.VMEM((rows * members, units), jnp.bfloat16),
        in_specs=[anywhere] * 8,
        out_specs=vmem,
        scratch_shapes=[
            pltpu.SMEM((hot_count * batch_size,), jnp.int32),
            pltpu.SMEM(table_of_feature.shape, jnp.int32),
            pltpu.VMEM((vocab, embed), jnp.bfloat16),
            pltpu.VMEM((vocab, embed), jnp.float32),
            pltpu.VMEM((rows, embed), jnp.float32),
            pltpu.VMEM((groups, rows, embed), jnp.bfloat16),
            pltpu.VMEM((members, groups, rows, embed), jnp.bfloat16),
            pltpu.VMEM((members, rows * members, block), jnp.bfloat16),
            pltpu.VMEM((members, rows * members, block), jnp.bfloat16),
            pltpu.VMEM((layers, width, rank), jnp.bfloat16),
            pltpu.VMEM((layers, block, rank), jnp.bfloat16),
            pltpu.VMEM((layers, members, rank, block), jnp.bfloat16),
            pltpu.VMEM((members, layers, block), jnp.float32),
            pltpu.VMEM((width, units), jnp.bfloat16),
            pltpu.VMEM((1, units), jnp.float32),
            dma((6 + pieces,)),
            dma((6,)),
            dma((pieces, members - 1)),
            dma((pieces, members - 1)),
            dma((pieces, members - 1)),
            dma((pieces, members - 1)),
            dma((3,)),
            dma((1,)),
            dma((members,)),
            dma((1,)),
        ],
        compiler_params=pltpu.CompilerParams(
            collective_id=0, has_side_effects=True, vmem_limit_bytes=VMEM_BYTES
        ),
    )(
        feature_ids[0].reshape(-1, LANES, hot_count).transpose(0, 2, 1).reshape(-1),
        table_of_feature,
        tables,
        cross_down,
        cross_up,
        cross_bias,
        tower_weight,
        tower_bias.reshape(1, -1),
    )


def body(
    feature_ids,
    tables,
    table_of_feature,
    cross_down,
    cross_up,
    cross_bias,
    tower_weight,
    tower_bias,
):
    groups = lax.axis_size("dp")
    members = lax.axis_size("mp")
    held = 2 * members * (cross_down.size + cross_up.size) + 2 * groups * tower_weight.size
    placed = groups == 2 * CHIPS and members == PLANES
    even = feature_ids.shape[1] % LANES == 0
    fits = held <= KERNEL_BYTES and placed and even and tables.shape[0] == 1
    chosen = fused_body if fits else plain_body
    return chosen(
        feature_ids,
        tables,
        table_of_feature,
        cross_down,
        cross_up,
        cross_bias,
        tower_weight,
        tower_bias,
    )


def solution(mesh):
    return jax.shard_map(
        body,
        mesh=mesh,
        in_specs=(
            P("dp", None, None),
            P("dp", None, None),
            P(),
            P(None, "mp", None),
            P(None, "mp", None),
            P(None, "mp"),
            P("dp", "mp"),
            P("mp"),
        ),
        out_specs=P("dp", "mp"),
        check_vma=False,
    )
```

```python
import functools

import jax
import jax.numpy as jnp
from jax import lax
from jax.experimental import pallas as pl
from jax.experimental.pallas import tpu as pltpu
from jax.sharding import PartitionSpec as P


def plain_body(
    feature_ids,
    tables,
    table_of_feature,
    cross_down,
    cross_up,
    cross_bias,
    tower_weight,
    tower_bias,
):
    groups = lax.axis_size("dp")
    members = lax.axis_size("mp")
    member = lax.axis_index("mp")
    table_count, batch_size, hot_count = feature_ids.shape
    row_count = batch_size // (groups * members)
    shaped = feature_ids[0].reshape(groups, members, row_count, hot_count)
    own_ids = lax.dynamic_index_in_dim(shaped, member, 1, keepdims=False).reshape(
        groups * row_count, hot_count
    )
    summed = jnp.zeros((groups * row_count, tables.shape[2]), jnp.float32)
    for hot_index in range(hot_count):
        summed = summed + jnp.take(tables[0], own_ids[:, hot_index], axis=0).astype(jnp.float32)
    columns = [summed.astype(jnp.bfloat16)]
    pooled = jnp.stack(columns, axis=1)
    regrouped = lax.all_to_all(pooled, "dp", split_axis=0, concat_axis=1, tiled=True)
    ordered = jnp.take(regrouped, table_of_feature, axis=1)
    by_width = lax.all_to_all(ordered, "mp", split_axis=1, concat_axis=0, tiled=True)
    group_rows = by_width.shape[0]
    embedded = by_width.reshape(group_rows, -1)
    embedded_wide = embedded.astype(jnp.float32)
    crossed = embedded
    layer_total = cross_down.shape[0]
    for layer_index in range(layer_total):
        partial_value = jnp.dot(
            crossed, cross_down[layer_index], preferred_element_type=jnp.float32
        )
        projected = lax.psum(partial_value.astype(jnp.bfloat16), "mp")
        lifted = lax.dot_general(
            projected,
            cross_up[layer_index],
            (((1,), (1,)), ((), ())),
            preferred_element_type=jnp.float32,
        )
        crossed = (
            embedded_wide * (lifted + cross_bias[layer_index]) + crossed.astype(jnp.float32)
        ).astype(jnp.bfloat16)
    full_rows = lax.all_gather(crossed, "mp", axis=1, tiled=True)
    pre_act = jnp.dot(
        full_rows,
        lax.all_gather(tower_weight, "dp", axis=0, tiled=True),
        preferred_element_type=jnp.float32,
    )
    return jax.nn.relu(pre_act + tower_bias).astype(jnp.bfloat16)


MESH = pl.DeviceIdType.MESH
KERNEL_BYTES = 24 * 1024 * 1024
VMEM_BYTES = (64 * 1024 - 352) * 1024
CHIPS = 4
PLANES = 4
LANES = 128
STEPS = (1, 3, 2)
FIRST = (
    "flip", "widen", "P6", "L1", "L2", "L3", "P7", "A6", "P4", "A7", "P5", "A4", "P2", "A5",
    "P3", "A2", "P1", "A3", "P0", "A1",
)
INNER = (
    "S0", "T1", "T2", "S3", "T4", "T5", "G1", "R0", "S6", "T7", "T8", "G0", "S9", "T10", "T11",
    "H1", "H0", "R1", "R2", "R3", "F11", "R4", "R5", "F10", "F01", "R6", "R7", "R8", "R9",
    "F00", "R10", "R11", "WR", "C0", "C1", "C2", "C3", "C4", "C5",
)
OUTER = (
    "S0", "S3", "S6", "S9", "G1", "H1", "G0", "H0", "S1", "S2", "R0", "S4", "S5", "R3", "S7",
    "S8", "R6", "S10", "S11", "R9", "R1", "R2", "R4", "R5", "R7", "R8", "R10", "R11", "WR",
    "C0", "C3", "C1", "C2", "C4", "C5",
)
LAST = (
    "C6", "C7", "C8", "C9", "C10", "C11", "E", "X0", "WC", "Y", "X1", "Z", "near", "end",
)


def kernel(
    groups,
    members,
    ids_hbm,
    order_hbm,
    table,
    down,
    up,
    bias,
    tower,
    tower_bias_hbm,
    out,
    ids,
    order,
    table_half,
    table_wide,
    sums,
    outbox,
    pooled,
    embedded,
    crossed,
    weights,
    up_raw,
    lifts,
    biases,
    tower_all,
    tower_bias,
    local_sem,
    send_sem,
    z_recv,
    plane_recv,
    diag_recv,
    pair_recv,
    tower_recv,
    pool_recv,
    share_recv,
    bias_recv,
):
    d = lax.axis_index("dp")
    m = lax.axis_index("mp")
    q = lax.div(d, 2)
    c = lax.rem(d, 2)
    partner = q * 2 + 1 - c
    chip_x = q + 1 - 2 * lax.rem(q, 2)
    chip_y = lax.rem(q + 2, CHIPS)
    chip_z = lax.rem(chip_x + 2, CHIPS)
    chips = (chip_x, chip_y, chip_z)
    layers, block, rank = down.shape
    rows, embed = sums.shape
    hots = ids.shape[0] // (rows * groups * members)
    piece = block // groups
    depth = tower.shape[0]
    pieces = 2 * layers
    others = members - 1

    def wrap(value, size):
        return lax.rem(value + size, size)

    def load(src, dst, index):
        copy = pltpu.make_async_copy(src, dst, local_sem.at[index])
        copy.start()
        return copy

    def remote(src, dst, which, recv_sem, to_d, to_m):
        return pltpu.make_async_remote_copy(
            src_ref=src,
            dst_ref=dst,
            send_sem=send_sem.at[which],
            recv_sem=recv_sem,
            device_id=(to_d, to_m),
            device_id_type=MESH,
        )

    def send(src, dst, which, recv_sem, to_d, to_m):
        remote(src, dst, which, recv_sem, to_d, to_m).start()

    def arrived(ref, recv_sem):
        remote(ref, ref, 0, recv_sem, partner, m).wait_recv()

    half_of = lax.div(m, 2)
    beside = m + 1 - 2 * lax.rem(m, 2)
    across = 2 - half_of
    far_first = 2 * (1 - half_of)
    inner = jnp.logical_or(m == 1, m == 2)
    outermost = 3 * (1 - half_of)

    def came(k):
        return (m, beside, across, outermost)[k]

    def goes(k):
        return wrap(m + k, members)

    thin = rank // groups

    def slot(p, member, device, half=None):
        full = piece if p % 2 == 0 else thin
        length = full if half is None else full // 2
        start = device * full + (0 if half is None else half * length)
        if p % 2 == 0:
            start = member * block + start
            return weights.at[p // 2, pl.ds(pl.multiple_of(start, length), length), :]
        return lifts.at[p // 2, member, pl.ds(pl.multiple_of(start, length), length), :]

    def amount(p, count):
        if p % 2 == 0:
            return weights.at[p // 2, pl.ds(0, count * piece), :]
        return lifts.at[p // 2, 0, pl.ds(0, count * thin), :]

    def tower_slot(device, half=None):
        length = depth if half is None else depth // 2
        start = device * depth + (0 if half is None else half * length)
        return tower_all.at[pl.ds(pl.multiple_of(start, length), length), :]

    barrier = pltpu.get_barrier_semaphore()
    for k in range(1, members):
        pl.semaphore_signal(barrier, inc=1, device_id=(d, goes(k)), device_id_type=MESH)
    for i in range(1, groups):
        pl.semaphore_signal(barrier, inc=1, device_id=(wrap(d + i, groups), m), device_id_type=MESH)

    here = pl.ds(pl.multiple_of(m * block, block), block)
    tower_copy = load(tower, tower_slot(d), 0)
    weight_copies = [load(down.at[n], weights.at[n, here, :], 1 + n) for n in range(layers)]
    up_copies = [load(up.at[n], up_raw.at[n], 1 + layers + n) for n in range(layers)]
    table_copy = load(table.at[0], table_half, pieces + 1)
    ids_copy = load(ids_hbm, ids, pieces + 2)
    bias_copy = load(bias, biases.at[m], pieces + 3)
    order_copy = load(order_hbm, order, pieces + 4)
    tower_bias_copy = load(tower_bias_hbm, tower_bias, pieces + 5)

    place = 3 - lax.rem(m + half_of, 2)

    def lend(p):
        mine = slot(p, m, d)
        send(mine, mine, p % 2, z_recv.at[p, place - 1], d, across)
        send(mine, mine, p % 2, z_recv.at[p, 0], d, beside)

    def spread(p, k):
        mine = slot(p, came(k), d)
        arrived(mine, z_recv.at[p, k - 1])
        send(mine, mine, p % 2, plane_recv.at[p, k - 1], chip_x * 2 + c, m)
        send(mine, mine, p % 2, plane_recv.at[p, k - 1], chip_y * 2 + c, m)
        send(mine, mine, p % 2, pair_recv.at[p, k - 1], partner, m)

    def pass_and_spread(p, k):
        mine = slot(p, came(k), d)
        arrived(mine, z_recv.at[p, k - 1])
        send(mine, mine, p % 2, z_recv.at[p, k - 1], d, beside)
        send(mine, mine, p % 2, plane_recv.at[p, k - 1], chip_x * 2 + c, m)
        send(mine, mine, p % 2, plane_recv.at[p, k - 1], chip_y * 2 + c, m)
        send(mine, mine, p % 2, pair_recv.at[p, k - 1], partner, m)

    def relay(p, k):
        arrived(amount(p, 2), plane_recv.at[p, k - 1])
        for j in range(2):
            half = slot(p, came(k), chips[j] * 2 + c, j)
            send(half, half, p % 2, diag_recv.at[p, k - 1], chips[1 - j] * 2 + c, m)
        for j in range(2):
            whole = slot(p, came(k), chips[j] * 2 + c)
            send(whole, whole, p % 2, pair_recv.at[p, k - 1], partner, m)

    def corner(p, k):
        far = slot(p, came(k), chip_z * 2 + c)
        arrived(far, diag_recv.at[p, k - 1])
        send(far, far, p % 2, pair_recv.at[p, k - 1], partner, m)

    def complete(p, k):
        arrived(amount(p, CHIPS), pair_recv.at[p, k - 1])

    def tower_spread():
        mine = tower_slot(d)
        send(mine, mine, 2, tower_recv.at[0], chip_x * 2 + c, m)
        send(mine, mine, 2, tower_recv.at[0], chip_y * 2 + c, m)
        send(mine, mine, 2, tower_recv.at[2], partner, m)

    def tower_relay():
        arrived(tower_all.at[pl.ds(0, 2 * depth), :], tower_recv.at[0])
        for j in range(2):
            half = tower_slot(chips[j] * 2 + c, j)
            send(half, half, 2, tower_recv.at[1], chips[1 - j] * 2 + c, m)
        for j in range(2):
            whole = tower_slot(chips[j] * 2 + c)
            send(whole, whole, 2, tower_recv.at[2], partner, m)

    def tower_corner():
        far = tower_slot(chip_z * 2 + c)
        arrived(far, tower_recv.at[1])
        send(far, far, 2, tower_recv.at[3], partner, m)

    step = 16 if rows % 16 == 0 else 8

    def pool(group):
        first = (group * members + m) * rows

        def some(index, carry):
            base = pl.multiple_of(index * step, step)
            lane = first + base
            word = lax.div(lane, LANES) * (LANES * hots) + lax.rem(lane, LANES)
            for r in range(step):
                total = None
                for hot in range(hots):
                    at = ids[word + (hot * LANES + r)]
                    row = table_wide[pl.ds(at, 1), :]
                    total = row if total is None else total + row
                sums[pl.ds(base + r, 1), :] = total
            return carry

        lax.fori_loop(0, rows // step, some, 0)
        return sums[...].astype(jnp.bfloat16)

    def related(j):
        return (q, chip_x, chip_y, chip_z)[j // 2] * 2 + (c if j % 2 == 0 else 1 - c)

    def pool_out(j):
        if j == 0:
            pooled[m, 0] = pool(d)
        else:
            outbox[j] = pool(related(j))

    def pool_away(j):
        send(outbox.at[j], pooled.at[m, j], 3, pool_recv.at[j // CHIPS], related(j), m)

    def part(quarter, half):
        return pooled.at[quarter, pl.ds(half * CHIPS, CHIPS)]

    def share_across(half):
        arrived(outbox.at[pl.ds(0, CHIPS - 1 + half)], pool_recv.at[half])
        mine = part(m, half)
        send(mine, mine, 4, share_recv.at[m, half], d, across)

    def share_beside(half):
        mine = part(m, half)
        send(mine, mine, 4, share_recv.at[m, half], d, beside)

    def pass_on(far, half):
        quarter = m + 2 - 4 * half_of if far else 3 - m
        theirs = part(quarter, half)
        arrived(theirs, share_recv.at[quarter, half])
        send(theirs, theirs, 4, share_recv.at[quarter, half], d, beside)

    def shared():
        for half in range(2):
            arrived(part(beside, half), share_recv.at[beside, half])

        @pl.when(jnp.logical_not(inner))
        def _():
            for j in range(2):
                for half in range(2):
                    arrived(part(far_first + j, half), share_recv.at[far_first + j, half])

    def embed_all():
        per_block = block // embed
        order_copy.wait()
        for b in range(members):
            for f in range(per_block):
                at = lax.bitwise_xor(order[b * per_block + f], d)
                for quarter in range(members):
                    embedded[
                        b, quarter * rows : (quarter + 1) * rows, f * embed : (f + 1) * embed
                    ] = pooled[quarter, at]

    def project(layer):
        state = embedded if layer == 0 else crossed
        value = None
        for b in range(members):
            term = jnp.dot(
                state[b],
                weights[layer, b * block : (b + 1) * block, :],
                preferred_element_type=jnp.float32,
            )
            value = term if value is None else value + term
        return value.astype(jnp.bfloat16)

    def lift(layer, projected, b):
        state = embedded if layer == 0 else crossed
        lifted = jnp.dot(projected, lifts[layer, b], preferred_element_type=jnp.float32)
        wide = embedded[b].astype(jnp.float32)
        value = wide * (lifted + biases[b, layer : layer + 1, :]) + state[b].astype(jnp.float32)
        return value.astype(jnp.bfloat16)

    units = [(p, k) for p in range(pieces) for k in STEPS]

    def do(call, *args):
        with jax.named_scope(call.__name__ + "_".join(map(str, args))):
            return call(*args)

    def first_sends():
        tower_copy.wait()
        pl.semaphore_wait(barrier, members - 1 + groups - 1)
        tower_spread()
        weight_copies[0].wait()
        lend(0)
        bias_copy.wait()
        for k in range(1, members):
            send(biases.at[m], biases.at[m], 5, bias_recv.at[0], d, goes(k))
        for copy in weight_copies[1:]:
            copy.wait()

    def flip():
        for n in range(layers):
            up_copies[n].wait()
            lifts[n, m] = up_raw[n].T

    def widen():
        table_copy.wait()
        table_wide[...] = table_half[...].astype(jnp.float32)
        ids_copy.wait()

    state = {}

    def ready():
        shared()
        embed_all()
        arrived(biases.at[pl.ds(0, others)], bias_recv.at[0])

    def narrow(layer):
        for k in STEPS:
            complete(2 * layer, k)
        state["projected"] = project(layer)

    def lift_first():
        for k in STEPS:
            complete(1, k)
        for b in range(members):
            crossed[b] = lift(0, state["projected"], b)

    def lift_last():
        for k in STEPS:
            complete(pieces - 1, k)
        for b in range(members):
            crossed[b] = lift(layers - 1, state["projected"], b)

    def tower_term(b):
        rows_of = pl.ds(pl.multiple_of(b * block, block), block)
        return jnp.dot(crossed[b], tower_all[rows_of, :], preferred_element_type=jnp.float32)

    def near_terms():
        tower_bias_copy.wait()
        arrived(tower_all.at[pl.ds(0, (CHIPS - 1) * depth), :], tower_recv.at[2])
        state["total"] = tower_term(q) + tower_term(chip_x) + tower_term(chip_y)

    def finish():
        arrived(tower_slot(chip_z * 2 + 1 - c), tower_recv.at[3])
        total = state["total"] + tower_term(chip_z)
        out[...] = jnp.maximum(total + tower_bias[...], 0.0).astype(jnp.bfloat16)

    def sent(ref, which):
        remote(ref, ref, which, bias_recv.at[0], partner, m).wait_send()

    def all_sent():
        total = others * (groups - 1) + 2
        sent(weights.at[:, pl.ds(0, total * piece), :], 0)
        sent(weights.at[:, pl.ds(0, total * piece), :], 1)
        sent(tower_all.at[pl.ds(0, 7 * depth), :], 2)
        sent(outbox.at[pl.ds(0, groups - 1)], 3)
        sent(pooled.at[pl.ds(0, 2)], 4)

        @pl.when(inner)
        def _():
            sent(weights.at[:, pl.ds(0, 2 * piece), :], 0)
            sent(weights.at[:, pl.ds(0, 2 * piece), :], 1)
            sent(pooled.at[pl.ds(0, 2)], 4)

        sent(biases.at[pl.ds(0, others)], 5)

    calls = {
        "P": pool_out,
        "A": pool_away,
        "L": lend,
        "F": pass_on,
        "G": share_across,
        "H": share_beside,
        "X": narrow,
    }
    on_units = {"S": spread, "T": pass_and_spread, "R": relay, "C": corner}
    words = {
        "flip": flip,
        "widen": widen,
        "WR": tower_relay,
        "WC": tower_corner,
        "E": ready,
        "Y": lift_first,
        "Z": lift_last,
        "near": near_terms,
        "end": finish,
    }
    def follow(plan):
        for word in plan:
            if word in words:
                do(words[word])
            elif word[0] in on_units:
                do(on_units[word[0]], *units[int(word[1:])])
            else:
                do(calls[word[0]], *map(int, word[1:]))

    do(first_sends)
    follow(FIRST)

    @pl.when(inner)
    def _():
        follow(INNER)

    @pl.when(jnp.logical_not(inner))
    def _():
        follow(OUTER)

    follow(LAST)
    do(all_sent)


def fused_body(
    feature_ids,
    tables,
    table_of_feature,
    cross_down,
    cross_up,
    cross_bias,
    tower_weight,
    tower_bias,
):
    groups = lax.axis_size("dp")
    members = lax.axis_size("mp")
    _, batch_size, hot_count = feature_ids.shape
    rows = batch_size // (groups * members)
    _, vocab, embed = tables.shape
    layers, block, rank = cross_down.shape
    depth, units = tower_weight.shape
    width = block * members
    pieces = 2 * layers
    dma = pltpu.SemaphoreType.DMA
    anywhere = pl.BlockSpec(memory_space=pl.ANY)
    vmem = pl.BlockSpec(memory_space=pltpu.VMEM)
    return pl.pallas_call(
        functools.partial(kernel, groups, members),
        out_shape=pltpu.VMEM((rows * members, units), jnp.bfloat16),
        in_specs=[anywhere] * 8,
        out_specs=vmem,
        scratch_shapes=[
            pltpu.SMEM((hot_count * batch_size,), jnp.int32),
            pltpu.SMEM(table_of_feature.shape, jnp.int32),
            pltpu.VMEM((vocab, embed), jnp.bfloat16),
            pltpu.VMEM((vocab, embed), jnp.float32),
            pltpu.VMEM((rows, embed), jnp.float32),
            pltpu.VMEM((groups, rows, embed), jnp.bfloat16),
            pltpu.VMEM((members, groups, rows, embed), jnp.bfloat16),
            pltpu.VMEM((members, rows * members, block), jnp.bfloat16),
            pltpu.VMEM((members, rows * members, block), jnp.bfloat16),
            pltpu.VMEM((layers, width, rank), jnp.bfloat16),
            pltpu.VMEM((layers, block, rank), jnp.bfloat16),
            pltpu.VMEM((layers, members, rank, block), jnp.bfloat16),
            pltpu.VMEM((members, layers, block), jnp.float32),
            pltpu.VMEM((width, units), jnp.bfloat16),
            pltpu.VMEM((1, units), jnp.float32),
            dma((6 + pieces,)),
            dma((6,)),
            dma((pieces, members - 1)),
            dma((pieces, members - 1)),
            dma((pieces, members - 1)),
            dma((pieces, members - 1)),
            dma((4,)),
            dma((2,)),
            dma((members, 2)),
            dma((1,)),
        ],
        compiler_params=pltpu.CompilerParams(
            collective_id=0, has_side_effects=True, vmem_limit_bytes=VMEM_BYTES
        ),
    )(
        feature_ids[0].reshape(-1, LANES, hot_count).transpose(0, 2, 1).reshape(-1),
        table_of_feature,
        tables,
        cross_down,
        cross_up,
        cross_bias,
        tower_weight,
        tower_bias.reshape(1, -1),
    )


def body(
    feature_ids,
    tables,
    table_of_feature,
    cross_down,
    cross_up,
    cross_bias,
    tower_weight,
    tower_bias,
):
    groups = lax.axis_size("dp")
    members = lax.axis_size("mp")
    held = 2 * members * (cross_down.size + cross_up.size) + 2 * groups * tower_weight.size
    placed = groups == 2 * CHIPS and members == PLANES
    even = feature_ids.shape[1] % LANES == 0
    fits = held <= KERNEL_BYTES and placed and even and tables.shape[0] == 1
    chosen = fused_body if fits else plain_body
    return chosen(
        feature_ids,
        tables,
        table_of_feature,
        cross_down,
        cross_up,
        cross_bias,
        tower_weight,
        tower_bias,
    )


def solution(mesh):
    return jax.shard_map(
        body,
        mesh=mesh,
        in_specs=(
            P("dp", None, None),
            P("dp", None, None),
            P(),
            P(None, "mp", None),
            P(None, "mp", None),
            P(None, "mp"),
            P("dp", "mp"),
            P("mp"),
        ),
        out_specs=P("dp", "mp"),
        check_vma=False,
    )
```

```python
import functools

import jax
import jax.numpy as jnp
from jax import lax
from jax.experimental import pallas as pl
from jax.experimental.pallas import tpu as pltpu
from jax.sharding import PartitionSpec as P


def plain_body(
    feature_ids,
    tables,
    table_of_feature,
    cross_down,
    cross_up,
    cross_bias,
    tower_weight,
    tower_bias,
):
    groups = lax.axis_size("dp")
    members = lax.axis_size("mp")
    member = lax.axis_index("mp")
    table_count, batch_size, hot_count = feature_ids.shape
    row_count = batch_size // (groups * members)
    shaped = feature_ids[0].reshape(groups, members, row_count, hot_count)
    own_ids = lax.dynamic_index_in_dim(shaped, member, 1, keepdims=False).reshape(
        groups * row_count, hot_count
    )
    summed = jnp.zeros((groups * row_count, tables.shape[2]), jnp.float32)
    for hot_index in range(hot_count):
        summed = summed + jnp.take(tables[0], own_ids[:, hot_index], axis=0).astype(jnp.float32)
    columns = [summed.astype(jnp.bfloat16)]
    pooled = jnp.stack(columns, axis=1)
    regrouped = lax.all_to_all(pooled, "dp", split_axis=0, concat_axis=1, tiled=True)
    ordered = jnp.take(regrouped, table_of_feature, axis=1)
    by_width = lax.all_to_all(ordered, "mp", split_axis=1, concat_axis=0, tiled=True)
    group_rows = by_width.shape[0]
    embedded = by_width.reshape(group_rows, -1)
    embedded_wide = embedded.astype(jnp.float32)
    crossed = embedded
    layer_total = cross_down.shape[0]
    for layer_index in range(layer_total):
        partial_value = jnp.dot(
            crossed, cross_down[layer_index], preferred_element_type=jnp.float32
        )
        projected = lax.psum(partial_value.astype(jnp.bfloat16), "mp")
        lifted = lax.dot_general(
            projected,
            cross_up[layer_index],
            (((1,), (1,)), ((), ())),
            preferred_element_type=jnp.float32,
        )
        crossed = (
            embedded_wide * (lifted + cross_bias[layer_index]) + crossed.astype(jnp.float32)
        ).astype(jnp.bfloat16)
    full_rows = lax.all_gather(crossed, "mp", axis=1, tiled=True)
    pre_act = jnp.dot(
        full_rows,
        lax.all_gather(tower_weight, "dp", axis=0, tiled=True),
        preferred_element_type=jnp.float32,
    )
    return jax.nn.relu(pre_act + tower_bias).astype(jnp.bfloat16)


MESH = pl.DeviceIdType.MESH
KERNEL_BYTES = 24 * 1024 * 1024
VMEM_BYTES = (64 * 1024 - 352) * 1024
CHIPS = 4
PLANES = 4
LANES = 128
STEPS = (1, 3, 2)
FIRST = (
    "flip", "widen", "P6", "L1", "L2", "L3", "P7", "A6", "P4", "A7", "P5", "A4", "P2", "A5",
)
INNER = (
    "P3", "A2", "P1", "A3", "T1", "T2", "P0", "A1", "S0", "T4", "T5", "S3", "G1", "T7", "T8",
    "G0", "S6", "T10", "T11", "S9", "H1", "H0", "R0", "R1", "R2", "R3", "F11", "R4", "R5",
    "F10", "F01", "R6", "R7", "R8", "R9", "F00", "R10", "R11", "WR", "C0", "C1",
)
OUTER = (
    "P3", "A2", "S0", "P1", "A3", "S3", "P0", "A1", "S6", "S9", "G1", "H1", "G0", "H0", "S1",
    "S2", "R0", "S4", "S5", "R3", "S7", "S8", "R6", "S10", "S11", "R9", "R1", "R2", "R4", "R5",
    "R7", "R8", "R10", "R11", "WR", "C0", "C1",
)
LAST = (
    "C2", "C3", "E", "X0", "Y", "WC", "X1", "Z", "near", "end",
)


def kernel(
    groups,
    members,
    ids_hbm,
    order_hbm,
    table,
    down,
    up,
    bias,
    tower,
    tower_bias_hbm,
    out,
    ids,
    order,
    table_half,
    table_wide,
    sums,
    outbox,
    pooled,
    embedded,
    crossed,
    weights,
    up_raw,
    lifts,
    biases,
    tower_all,
    tower_bias,
    local_sem,
    send_sem,
    z_recv,
    plane_recv,
    diag_recv,
    pair_recv,
    tower_recv,
    pool_recv,
    share_recv,
    bias_recv,
):
    d = lax.axis_index("dp")
    m = lax.axis_index("mp")
    q = lax.div(d, 2)
    c = lax.rem(d, 2)
    partner = q * 2 + 1 - c
    chip_x = q + 1 - 2 * lax.rem(q, 2)
    chip_y = lax.rem(q + 2, CHIPS)
    chip_z = lax.rem(chip_x + 2, CHIPS)
    chips = (chip_x, chip_y, chip_z)
    layers, block, rank = down.shape
    rows, embed = sums.shape
    hots = ids.shape[0] // (rows * groups * members)
    piece = block // groups
    depth = tower.shape[0]
    pieces = 2 * layers
    others = members - 1

    def wrap(value, size):
        return lax.rem(value + size, size)

    def load(src, dst, index):
        copy = pltpu.make_async_copy(src, dst, local_sem.at[index])
        copy.start()
        return copy

    def remote(src, dst, which, recv_sem, to_d, to_m):
        return pltpu.make_async_remote_copy(
            src_ref=src,
            dst_ref=dst,
            send_sem=send_sem.at[which],
            recv_sem=recv_sem,
            device_id=(to_d, to_m),
            device_id_type=MESH,
        )

    def send(src, dst, which, recv_sem, to_d, to_m):
        remote(src, dst, which, recv_sem, to_d, to_m).start()

    def arrived(ref, recv_sem):
        remote(ref, ref, 0, recv_sem, partner, m).wait_recv()

    half_of = lax.div(m, 2)
    beside = m + 1 - 2 * lax.rem(m, 2)
    across = 2 - half_of
    far_first = 2 * (1 - half_of)
    inner = jnp.logical_or(m == 1, m == 2)
    outermost = 3 * (1 - half_of)

    def came(k):
        return (m, beside, across, outermost)[k]

    def goes(k):
        return wrap(m + k, members)

    thin = rank // groups

    def slot(p, member, device, half=None):
        full = piece if p % 2 == 0 else thin
        length = full if half is None else full // 2
        start = device * full + (0 if half is None else half * length)
        if p % 2 == 0:
            start = member * block + start
            return weights.at[p // 2, pl.ds(pl.multiple_of(start, length), length), :]
        return lifts.at[p // 2, member, pl.ds(pl.multiple_of(start, length), length), :]

    def amount(count):
        return weights.at[0, pl.ds(0, count * piece), :]

    def tower_slot(device, half=None):
        length = depth if half is None else depth // 2
        start = device * depth + (0 if half is None else half * length)
        return tower_all.at[pl.ds(pl.multiple_of(start, length), length), :]

    barrier = pltpu.get_barrier_semaphore()
    for k in range(1, members):
        pl.semaphore_signal(barrier, inc=1, device_id=(d, goes(k)), device_id_type=MESH)
    for i in range(1, groups):
        pl.semaphore_signal(barrier, inc=1, device_id=(wrap(d + i, groups), m), device_id_type=MESH)

    here = pl.ds(pl.multiple_of(m * block, block), block)
    tower_copy = load(tower, tower_slot(d), 0)
    down_copy = load(down, weights.at[:, here, :], 1)
    up_copy = load(up, up_raw, 2)
    table_copy = load(table.at[0], table_half, 3)
    ids_copy = load(ids_hbm, ids, 4)
    bias_copy = load(bias, biases.at[m], 5)
    order_copy = load(order_hbm, order, 6)
    tower_bias_copy = load(tower_bias_hbm, tower_bias, 7)

    place = 3 - lax.rem(m + half_of, 2)

    def lend(p):
        mine = slot(p, m, d)
        send(mine, mine, p % 2, z_recv.at[p, place - 1], d, across)
        send(mine, mine, p % 2, z_recv.at[p, 0], d, beside)

    def spread(p, k):
        mine = slot(p, came(k), d)
        arrived(mine, z_recv.at[p, k - 1])
        send(mine, mine, p % 2, plane_recv.at[p, k - 1], chip_x * 2 + c, m)
        send(mine, mine, p % 2, plane_recv.at[p, k - 1], chip_y * 2 + c, m)
        send(mine, mine, p % 2, pair_recv.at[p], partner, m)

    def pass_and_spread(p, k):
        mine = slot(p, came(k), d)
        arrived(mine, z_recv.at[p, k - 1])
        send(mine, mine, p % 2, z_recv.at[p, k - 1], d, beside)
        send(mine, mine, p % 2, plane_recv.at[p, k - 1], chip_x * 2 + c, m)
        send(mine, mine, p % 2, plane_recv.at[p, k - 1], chip_y * 2 + c, m)
        send(mine, mine, p % 2, pair_recv.at[p], partner, m)

    def relay(p, k):
        arrived(amount(2), plane_recv.at[p, k - 1])
        for j in range(2):
            half = slot(p, came(k), chips[j] * 2 + c, j)
            send(half, half, p % 2, diag_recv.at[p], chips[1 - j] * 2 + c, m)
        for j in range(2):
            whole = slot(p, came(k), chips[j] * 2 + c)
            send(whole, whole, p % 2, pair_recv.at[p], partner, m)

    def corner(p):
        arrived(amount(others), diag_recv.at[p])
        for k in STEPS:
            far = slot(p, came(k), chip_z * 2 + c)
            send(far, far, p % 2, pair_recv.at[p], partner, m)

    def complete(p):
        arrived(amount(CHIPS * others), pair_recv.at[p])

    def tower_spread():
        mine = tower_slot(d)
        send(mine, mine, 2, tower_recv.at[0], chip_x * 2 + c, m)
        send(mine, mine, 2, tower_recv.at[0], chip_y * 2 + c, m)
        send(mine, mine, 2, tower_recv.at[2], partner, m)

    def tower_relay():
        arrived(tower_all.at[pl.ds(0, 2 * depth), :], tower_recv.at[0])
        for j in range(2):
            half = tower_slot(chips[j] * 2 + c, j)
            send(half, half, 2, tower_recv.at[1], chips[1 - j] * 2 + c, m)
        for j in range(2):
            whole = tower_slot(chips[j] * 2 + c)
            send(whole, whole, 2, tower_recv.at[2], partner, m)

    def tower_corner():
        far = tower_slot(chip_z * 2 + c)
        arrived(far, tower_recv.at[1])
        send(far, far, 2, tower_recv.at[3], partner, m)

    step = 16 if rows % 16 == 0 else 8

    def pool(group):
        first = (group * members + m) * rows

        def some(index, carry):
            base = pl.multiple_of(index * step, step)
            lane = first + base
            word = lax.div(lane, LANES) * (LANES * hots) + lax.rem(lane, LANES)
            for r in range(step):
                total = None
                for hot in range(hots):
                    at = ids[word + (hot * LANES + r)]
                    row = table_wide[pl.ds(at, 1), :]
                    total = row if total is None else total + row
                sums[pl.ds(base + r, 1), :] = total
            return carry

        lax.fori_loop(0, rows // step, some, 0)
        return sums[...].astype(jnp.bfloat16)

    def related(j):
        return (q, chip_x, chip_y, chip_z)[j // 2] * 2 + (c if j % 2 == 0 else 1 - c)

    def pool_out(j):
        if j == 0:
            pooled[m, 0] = pool(d)
        else:
            outbox[j] = pool(related(j))

    def pool_away(j):
        send(outbox.at[j], pooled.at[m, j], 3, pool_recv.at[j // CHIPS], related(j), m)

    def part(quarter, half):
        return pooled.at[quarter, pl.ds(half * CHIPS, CHIPS)]

    def share_across(half):
        arrived(outbox.at[pl.ds(0, CHIPS - 1 + half)], pool_recv.at[half])
        mine = part(m, half)
        send(mine, mine, 4, share_recv.at[m, half], d, across)

    def share_beside(half):
        mine = part(m, half)
        send(mine, mine, 4, share_recv.at[m, half], d, beside)

    def pass_on(far, half):
        quarter = m + 2 - 4 * half_of if far else 3 - m
        theirs = part(quarter, half)
        arrived(theirs, share_recv.at[quarter, half])
        send(theirs, theirs, 4, share_recv.at[quarter, half], d, beside)

    def shared():
        for half in range(2):
            arrived(part(beside, half), share_recv.at[beside, half])

        @pl.when(jnp.logical_not(inner))
        def _():
            for j in range(2):
                for half in range(2):
                    arrived(part(far_first + j, half), share_recv.at[far_first + j, half])

    def embed_all():
        per_block = block // embed
        order_copy.wait()
        for b in range(members):
            for f in range(per_block):
                at = lax.bitwise_xor(order[b * per_block + f], d)
                for quarter in range(members):
                    embedded[
                        b, quarter * rows : (quarter + 1) * rows, f * embed : (f + 1) * embed
                    ] = pooled[quarter, at]

    def project(layer):
        state = embedded if layer == 0 else crossed
        value = None
        for b in range(members):
            term = jnp.dot(
                state[b],
                weights[layer, b * block : (b + 1) * block, :],
                preferred_element_type=jnp.float32,
            )
            value = term if value is None else value + term
        return value.astype(jnp.bfloat16)

    def lift(layer, projected, b):
        state = embedded if layer == 0 else crossed
        lifted = jnp.dot(projected, lifts[layer, b], preferred_element_type=jnp.float32)
        wide = embedded[b].astype(jnp.float32)
        value = wide * (lifted + biases[b, layer : layer + 1, :]) + state[b].astype(jnp.float32)
        return value.astype(jnp.bfloat16)

    units = [(p, k) for p in range(pieces) for k in STEPS]

    def do(call, *args):
        with jax.named_scope(call.__name__ + "_".join(map(str, args))):
            return call(*args)

    def first_sends():
        tower_copy.wait()
        pl.semaphore_wait(barrier, members - 1 + groups - 1)
        tower_spread()
        down_copy.wait()
        lend(0)
        bias_copy.wait()
        for k in range(1, members):
            send(biases.at[m], biases.at[m], 5, bias_recv.at[0], d, goes(k))

    def flip():
        up_copy.wait()
        for n in range(layers):
            lifts[n, m] = up_raw[n].T

    def widen():
        table_copy.wait()
        table_wide[...] = table_half[...].astype(jnp.float32)
        ids_copy.wait()

    state = {}

    def ready():
        shared()
        embed_all()
        arrived(biases.at[pl.ds(0, others)], bias_recv.at[0])

    def narrow(layer):
        complete(2 * layer)
        state["projected"] = project(layer)

    def lift_first():
        complete(1)
        for b in range(members):
            crossed[b] = lift(0, state["projected"], b)

    def lift_last():
        complete(pieces - 1)
        for b in range(members):
            crossed[b] = lift(layers - 1, state["projected"], b)

    def tower_term(b):
        rows_of = pl.ds(pl.multiple_of(b * block, block), block)
        return jnp.dot(crossed[b], tower_all[rows_of, :], preferred_element_type=jnp.float32)

    def near_terms():
        tower_bias_copy.wait()
        arrived(tower_all.at[pl.ds(0, (CHIPS - 1) * depth), :], tower_recv.at[2])
        state["total"] = tower_term(q) + tower_term(chip_x) + tower_term(chip_y)

    def finish():
        arrived(tower_slot(chip_z * 2 + 1 - c), tower_recv.at[3])
        total = state["total"] + tower_term(chip_z)
        out[...] = jnp.maximum(total + tower_bias[...], 0.0).astype(jnp.bfloat16)

    def sent(ref, which):
        remote(ref, ref, which, bias_recv.at[0], partner, m).wait_send()

    def all_sent():
        total = others * (groups - 1) + 2
        sent(weights.at[:, pl.ds(0, total * piece), :], 0)
        sent(weights.at[:, pl.ds(0, total * piece), :], 1)
        sent(tower_all.at[pl.ds(0, 7 * depth), :], 2)
        sent(outbox.at[pl.ds(0, groups - 1)], 3)
        sent(pooled.at[pl.ds(0, 2)], 4)

        @pl.when(inner)
        def _():
            sent(weights.at[:, pl.ds(0, 2 * piece), :], 0)
            sent(weights.at[:, pl.ds(0, 2 * piece), :], 1)
            sent(pooled.at[pl.ds(0, 2)], 4)

        sent(biases.at[pl.ds(0, others)], 5)

    calls = {
        "P": pool_out,
        "A": pool_away,
        "L": lend,
        "C": corner,
        "F": pass_on,
        "G": share_across,
        "H": share_beside,
        "X": narrow,
    }
    on_units = {"S": spread, "T": pass_and_spread, "R": relay}
    words = {
        "flip": flip,
        "widen": widen,
        "WR": tower_relay,
        "WC": tower_corner,
        "E": ready,
        "Y": lift_first,
        "Z": lift_last,
        "near": near_terms,
        "end": finish,
    }
    def follow(plan):
        for word in plan:
            if word in words:
                do(words[word])
            elif word[0] in on_units:
                do(on_units[word[0]], *units[int(word[1:])])
            else:
                do(calls[word[0]], *map(int, word[1:]))

    do(first_sends)
    follow(FIRST)

    @pl.when(inner)
    def _():
        follow(INNER)

    @pl.when(jnp.logical_not(inner))
    def _():
        follow(OUTER)

    follow(LAST)
    do(all_sent)


def fused_body(
    feature_ids,
    tables,
    table_of_feature,
    cross_down,
    cross_up,
    cross_bias,
    tower_weight,
    tower_bias,
):
    groups = lax.axis_size("dp")
    members = lax.axis_size("mp")
    _, batch_size, hot_count = feature_ids.shape
    rows = batch_size // (groups * members)
    _, vocab, embed = tables.shape
    layers, block, rank = cross_down.shape
    depth, units = tower_weight.shape
    width = block * members
    pieces = 2 * layers
    dma = pltpu.SemaphoreType.DMA
    anywhere = pl.BlockSpec(memory_space=pl.ANY)
    vmem = pl.BlockSpec(memory_space=pltpu.VMEM)
    return pl.pallas_call(
        functools.partial(kernel, groups, members),
        out_shape=pltpu.VMEM((rows * members, units), jnp.bfloat16),
        in_specs=[anywhere] * 8,
        out_specs=vmem,
        scratch_shapes=[
            pltpu.SMEM((hot_count * batch_size,), jnp.int32),
            pltpu.SMEM(table_of_feature.shape, jnp.int32),
            pltpu.VMEM((vocab, embed), jnp.bfloat16),
            pltpu.VMEM((vocab, embed), jnp.float32),
            pltpu.VMEM((rows, embed), jnp.float32),
            pltpu.VMEM((groups, rows, embed), jnp.bfloat16),
            pltpu.VMEM((members, groups, rows, embed), jnp.bfloat16),
            pltpu.VMEM((members, rows * members, block), jnp.bfloat16),
            pltpu.VMEM((members, rows * members, block), jnp.bfloat16),
            pltpu.VMEM((layers, width, rank), jnp.bfloat16),
            pltpu.VMEM((layers, block, rank), jnp.bfloat16),
            pltpu.VMEM((layers, members, rank, block), jnp.bfloat16),
            pltpu.VMEM((members, layers, block), jnp.float32),
            pltpu.VMEM((width, units), jnp.bfloat16),
            pltpu.VMEM((1, units), jnp.float32),
            dma((8,)),
            dma((6,)),
            dma((pieces, members - 1)),
            dma((pieces, members - 1)),
            dma((pieces,)),
            dma((pieces,)),
            dma((4,)),
            dma((2,)),
            dma((members, 2)),
            dma((1,)),
        ],
        compiler_params=pltpu.CompilerParams(
            collective_id=0, has_side_effects=True, vmem_limit_bytes=VMEM_BYTES
        ),
    )(
        feature_ids[0].reshape(-1, LANES, hot_count).transpose(0, 2, 1).reshape(-1),
        table_of_feature,
        tables,
        cross_down,
        cross_up,
        cross_bias,
        tower_weight,
        tower_bias.reshape(1, -1),
    )


def body(
    feature_ids,
    tables,
    table_of_feature,
    cross_down,
    cross_up,
    cross_bias,
    tower_weight,
    tower_bias,
):
    groups = lax.axis_size("dp")
    members = lax.axis_size("mp")
    held = 2 * members * (cross_down.size + cross_up.size) + 2 * groups * tower_weight.size
    placed = groups == 2 * CHIPS and members == PLANES
    even = feature_ids.shape[1] % LANES == 0
    fits = held <= KERNEL_BYTES and placed and even and tables.shape[0] == 1
    chosen = fused_body if fits else plain_body
    return chosen(
        feature_ids,
        tables,
        table_of_feature,
        cross_down,
        cross_up,
        cross_bias,
        tower_weight,
        tower_bias,
    )


def solution(mesh):
    return jax.shard_map(
        body,
        mesh=mesh,
        in_specs=(
            P("dp", None, None),
            P("dp", None, None),
            P(),
            P(None, "mp", None),
            P(None, "mp", None),
            P(None, "mp"),
            P("dp", "mp"),
            P("mp"),
        ),
        out_specs=P("dp", "mp"),
        check_vma=False,
    )
```

```python
import functools

import jax
import jax.numpy as jnp
from jax import lax
from jax.experimental import pallas as pl
from jax.experimental.pallas import tpu as pltpu
from jax.sharding import PartitionSpec as P


def plain_body(
    feature_ids,
    tables,
    table_of_feature,
    cross_down,
    cross_up,
    cross_bias,
    tower_weight,
    tower_bias,
):
    groups = lax.axis_size("dp")
    members = lax.axis_size("mp")
    member = lax.axis_index("mp")
    table_count, batch_size, hot_count = feature_ids.shape
    row_count = batch_size // (groups * members)
    shaped = feature_ids[0].reshape(groups, members, row_count, hot_count)
    own_ids = lax.dynamic_index_in_dim(shaped, member, 1, keepdims=False).reshape(
        groups * row_count, hot_count
    )
    summed = jnp.zeros((groups * row_count, tables.shape[2]), jnp.float32)
    for hot_index in range(hot_count):
        summed = summed + jnp.take(tables[0], own_ids[:, hot_index], axis=0).astype(jnp.float32)
    columns = [summed.astype(jnp.bfloat16)]
    pooled = jnp.stack(columns, axis=1)
    regrouped = lax.all_to_all(pooled, "dp", split_axis=0, concat_axis=1, tiled=True)
    ordered = jnp.take(regrouped, table_of_feature, axis=1)
    by_width = lax.all_to_all(ordered, "mp", split_axis=1, concat_axis=0, tiled=True)
    group_rows = by_width.shape[0]
    embedded = by_width.reshape(group_rows, -1)
    embedded_wide = embedded.astype(jnp.float32)
    crossed = embedded
    layer_total = cross_down.shape[0]
    for layer_index in range(layer_total):
        partial_value = jnp.dot(
            crossed, cross_down[layer_index], preferred_element_type=jnp.float32
        )
        projected = lax.psum(partial_value.astype(jnp.bfloat16), "mp")
        lifted = lax.dot_general(
            projected,
            cross_up[layer_index],
            (((1,), (1,)), ((), ())),
            preferred_element_type=jnp.float32,
        )
        crossed = (
            embedded_wide * (lifted + cross_bias[layer_index]) + crossed.astype(jnp.float32)
        ).astype(jnp.bfloat16)
    full_rows = lax.all_gather(crossed, "mp", axis=1, tiled=True)
    pre_act = jnp.dot(
        full_rows,
        lax.all_gather(tower_weight, "dp", axis=0, tiled=True),
        preferred_element_type=jnp.float32,
    )
    return jax.nn.relu(pre_act + tower_bias).astype(jnp.bfloat16)


MESH = pl.DeviceIdType.MESH
KERNEL_BYTES = 24 * 1024 * 1024
VMEM_BYTES = (64 * 1024 - 352) * 1024
CHIPS = 4
PLANES = 4
LANES = 128
STEPS = (1, 3, 2)
FIRST = (
    "flip", "widen", "P6", "L1", "L2", "L3", "P7", "A6", "P4", "A7", "P5", "A4", "P2", "A5",
)
INNER = (
    "P3", "A2", "P1", "A3", "T1", "T2", "P0", "A1", "S0", "T4", "T5", "S3", "G1", "T7", "T8",
    "G0", "S6", "T10", "T11", "S9", "H1", "H0", "WP", "R0", "R1", "R2", "R3", "F11", "R4", "R5",
    "F10", "F01", "R6", "R7", "R8", "R9", "F00", "R10", "R11", "WR", "C0", "C1",
)
OUTER = (
    "P3", "A2", "S0", "P1", "A3", "S3", "P0", "A1", "S6", "S9", "G1", "H1", "G0", "H0", "WP",
    "S1", "S2", "R0", "S4", "S5", "R3", "S7", "S8", "R6", "S10", "S11", "R9", "R1", "R2", "R4",
    "R5", "R7", "R8", "R10", "R11", "WR", "C0", "C1",
)
LAST = (
    "C2", "C3", "E", "X0", "Y", "WC", "X1", "Z", "end",
)


def kernel(
    groups,
    members,
    ids_hbm,
    order_hbm,
    table,
    down,
    up,
    bias,
    tower,
    tower_bias_hbm,
    out,
    ids,
    order,
    table_half,
    table_wide,
    sums,
    outbox,
    pooled,
    embedded,
    crossed,
    weights,
    up_raw,
    lifts,
    biases,
    tower_all,
    tower_bias,
    local_sem,
    send_sem,
    z_recv,
    plane_recv,
    diag_recv,
    pair_recv,
    tower_recv,
    pool_recv,
    share_recv,
    bias_recv,
):
    d = lax.axis_index("dp")
    m = lax.axis_index("mp")
    q = lax.div(d, 2)
    c = lax.rem(d, 2)
    partner = q * 2 + 1 - c
    chip_x = q + 1 - 2 * lax.rem(q, 2)
    chip_y = lax.rem(q + 2, CHIPS)
    chip_z = lax.rem(chip_x + 2, CHIPS)
    chips = (chip_x, chip_y, chip_z)
    layers, block, rank = down.shape
    rows, embed = sums.shape
    hots = ids.shape[0] // (rows * groups * members)
    piece = block // groups
    depth = tower.shape[0]
    pieces = 2 * layers
    others = members - 1

    def wrap(value, size):
        return lax.rem(value + size, size)

    def load(src, dst, index):
        copy = pltpu.make_async_copy(src, dst, local_sem.at[index])
        copy.start()
        return copy

    def remote(src, dst, which, recv_sem, to_d, to_m):
        return pltpu.make_async_remote_copy(
            src_ref=src,
            dst_ref=dst,
            send_sem=send_sem.at[which],
            recv_sem=recv_sem,
            device_id=(to_d, to_m),
            device_id_type=MESH,
        )

    def send(src, dst, which, recv_sem, to_d, to_m):
        remote(src, dst, which, recv_sem, to_d, to_m).start()

    def arrived(ref, recv_sem):
        remote(ref, ref, 0, recv_sem, partner, m).wait_recv()

    half_of = lax.div(m, 2)
    beside = m + 1 - 2 * lax.rem(m, 2)
    across = 2 - half_of
    far_first = 2 * (1 - half_of)
    inner = jnp.logical_or(m == 1, m == 2)
    outermost = 3 * (1 - half_of)

    def came(k):
        return (m, beside, across, outermost)[k]

    def goes(k):
        return wrap(m + k, members)

    thin = rank // groups

    def slot(p, member, device, half=None):
        full = piece if p % 2 == 0 else thin
        length = full if half is None else full // 2
        start = device * full + (0 if half is None else half * length)
        if p % 2 == 0:
            start = member * block + start
            return weights.at[p // 2, pl.ds(pl.multiple_of(start, length), length), :]
        return lifts.at[p // 2, member, pl.ds(pl.multiple_of(start, length), length), :]

    def amount(count):
        return weights.at[0, pl.ds(0, count * piece), :]

    def tower_slot(device, half=None):
        length = depth if half is None else depth // 2
        start = device * depth + (0 if half is None else half * length)
        return tower_all.at[pl.ds(pl.multiple_of(start, length), length), :]

    here = pl.ds(pl.multiple_of(m * block, block), block)
    tower_copy = load(tower, tower_slot(d), 0)
    down_copy = load(down, weights.at[:, here, :], 1)
    barrier = pltpu.get_barrier_semaphore()
    for k in range(1, members):
        pl.semaphore_signal(barrier, inc=1, device_id=(d, goes(k)), device_id_type=MESH)
    for i in range(1, groups):
        pl.semaphore_signal(barrier, inc=1, device_id=(wrap(d + i, groups), m), device_id_type=MESH)

    up_copy = load(up, up_raw, 2)
    table_copy = load(table.at[0], table_half, 3)
    ids_copy = load(ids_hbm, ids, 4)
    bias_copy = load(bias, biases.at[m], 5)
    order_copy = load(order_hbm, order, 6)
    tower_bias_copy = load(tower_bias_hbm, tower_bias, 7)

    place = 3 - lax.rem(m + half_of, 2)

    def lend(p):
        mine = slot(p, m, d)
        send(mine, mine, p % 2, z_recv.at[p, place - 1], d, across)
        send(mine, mine, p % 2, z_recv.at[p, 0], d, beside)

    def spread(p, k):
        mine = slot(p, came(k), d)
        arrived(mine, z_recv.at[p, k - 1])
        send(mine, mine, p % 2, plane_recv.at[p, k - 1], chip_x * 2 + c, m)
        send(mine, mine, p % 2, plane_recv.at[p, k - 1], chip_y * 2 + c, m)
        send(mine, mine, p % 2, pair_recv.at[p], partner, m)

    def pass_and_spread(p, k):
        mine = slot(p, came(k), d)
        arrived(mine, z_recv.at[p, k - 1])
        send(mine, mine, p % 2, z_recv.at[p, k - 1], d, beside)
        send(mine, mine, p % 2, plane_recv.at[p, k - 1], chip_x * 2 + c, m)
        send(mine, mine, p % 2, plane_recv.at[p, k - 1], chip_y * 2 + c, m)
        send(mine, mine, p % 2, pair_recv.at[p], partner, m)

    def relay(p, k):
        arrived(amount(2), plane_recv.at[p, k - 1])
        for j in range(2):
            half = slot(p, came(k), chips[j] * 2 + c, j)
            send(half, half, p % 2, diag_recv.at[p], chips[1 - j] * 2 + c, m)
        for j in range(2):
            whole = slot(p, came(k), chips[j] * 2 + c)
            send(whole, whole, p % 2, pair_recv.at[p], partner, m)

    def corner(p):
        arrived(amount(others), diag_recv.at[p])
        for k in STEPS:
            far = slot(p, came(k), chip_z * 2 + c)
            send(far, far, p % 2, pair_recv.at[p], partner, m)

    def complete(p):
        arrived(amount(CHIPS * others), pair_recv.at[p])

    def tower_spread():
        mine = tower_slot(d)
        send(mine, mine, 2, tower_recv.at[0], chip_x * 2 + c, m)
        send(mine, mine, 2, tower_recv.at[0], chip_y * 2 + c, m)
        send(mine, mine, 2, tower_recv.at[2], partner, m)

    def tower_pair():
        arrived(tower_all.at[pl.ds(0, 2 * depth), :], tower_recv.at[0])
        for j in range(2):
            whole = tower_slot(chips[j] * 2 + c)
            send(whole, whole, 2, tower_recv.at[2], partner, m)

    def tower_relay():
        @pl.when(c == 1)
        def _():
            arrived(tower_all.at[pl.ds(0, 3 * depth), :], tower_recv.at[2])
            for core in range(2):
                for j in range(2):
                    half = tower_slot(chips[j] * 2 + core, j)
                    send(half, half, 2, tower_recv.at[1], chips[1 - j] * 2 + c, m)

    def tower_corner():
        @pl.when(c == 1)
        def _():
            far = tower_all.at[pl.ds(pl.multiple_of(chip_z * block, block), block), :]
            arrived(far, tower_recv.at[1])
            send(far, far, 2, tower_recv.at[3], partner, m)

    step = 16 if rows % 16 == 0 else 8

    def pool(group):
        first = (group * members + m) * rows

        def some(index, carry):
            base = pl.multiple_of(index * step, step)
            lane = first + base
            word = lax.div(lane, LANES) * (LANES * hots) + lax.rem(lane, LANES)
            for r in range(step):
                total = None
                for hot in range(hots):
                    at = ids[word + (hot * LANES + r)]
                    row = table_wide[pl.ds(at, 1), :]
                    total = row if total is None else total + row
                sums[pl.ds(base + r, 1), :] = total
            return carry

        lax.fori_loop(0, rows // step, some, 0)
        return sums[...].astype(jnp.bfloat16)

    def related(j):
        return (q, chip_x, chip_y, chip_z)[j // 2] * 2 + (c if j % 2 == 0 else 1 - c)

    def pool_out(j):
        if j == 0:
            pooled[m, 0] = pool(d)
        else:
            outbox[j] = pool(related(j))

    def pool_away(j):
        send(outbox.at[j], pooled.at[m, j], 3, pool_recv.at[j // CHIPS], related(j), m)

    def part(quarter, half):
        return pooled.at[quarter, pl.ds(half * CHIPS, CHIPS)]

    def share_across(half):
        arrived(outbox.at[pl.ds(0, CHIPS - 1 + half)], pool_recv.at[half])
        mine = part(m, half)
        send(mine, mine, 4, share_recv.at[m, half], d, across)

    def share_beside(half):
        mine = part(m, half)
        send(mine, mine, 4, share_recv.at[m, half], d, beside)

    def pass_on(far, half):
        quarter = m + 2 - 4 * half_of if far else 3 - m
        theirs = part(quarter, half)
        arrived(theirs, share_recv.at[quarter, half])
        send(theirs, theirs, 4, share_recv.at[quarter, half], d, beside)

    def ready_all():
        for half in range(2):
            arrived(part(beside, half), share_recv.at[beside, half])

        @pl.when(jnp.logical_not(inner))
        def _():
            for quarter in (outermost, across):
                for half in range(2):
                    arrived(part(quarter, half), share_recv.at[quarter, half])

        order_copy.wait()
        arrived(biases.at[pl.ds(0, others)], bias_recv.at[0])
        for f in range(groups):
            at = lax.bitwise_xor(order[f], d)
            for quarter in range(members):
                here = slice(quarter * rows, (quarter + 1) * rows)
                embedded[here, f * embed : (f + 1) * embed] = pooled[quarter, at]

    def project(layer):
        state = embedded if layer == 0 else crossed
        value = jnp.dot(state[...], weights[layer], preferred_element_type=jnp.float32)
        return value.astype(jnp.bfloat16)

    def lift(layer, projected, b):
        state = embedded if layer == 0 else crossed
        here = slice(b * block, (b + 1) * block)
        lifted = jnp.dot(projected, lifts[layer, b], preferred_element_type=jnp.float32)
        wide = embedded[:, here].astype(jnp.float32)
        value = wide * (lifted + biases[b, layer : layer + 1, :])
        crossed[:, here] = (value + state[:, here].astype(jnp.float32)).astype(jnp.bfloat16)

    units = [(p, k) for p in range(pieces) for k in STEPS]

    def do(call, *args):
        with jax.named_scope(call.__name__ + "_".join(map(str, args))):
            return call(*args)

    def first_sends():
        tower_copy.wait()
        pl.semaphore_wait(barrier, members - 1 + groups - 1)
        tower_spread()
        down_copy.wait()
        lend(0)
        bias_copy.wait()
        for k in range(1, members):
            send(biases.at[m], biases.at[m], 5, bias_recv.at[0], d, goes(k))

    def flip():
        up_copy.wait()
        for n in range(layers):
            lifts[n, m] = up_raw[n].T

    def widen():
        table_copy.wait()
        table_wide[...] = table_half[...].astype(jnp.float32)
        ids_copy.wait()

    state = {}

    def narrow(layer):
        complete(2 * layer)
        state["projected"] = project(layer)

    def lift_first():
        complete(1)
        for b in range(members):
            lift(0, state["projected"], b)

    def lift_last():
        complete(pieces - 1)
        for b in range(members):
            lift(layers - 1, state["projected"], b)

    def finish():
        tower_bias_copy.wait()

        @pl.when(c == 0)
        def _():
            arrived(tower_all.at[pl.ds(0, 3 * depth), :], tower_recv.at[2])
            arrived(tower_all.at[pl.ds(0, block), :], tower_recv.at[3])

        total = jnp.dot(crossed[...], tower_all[...], preferred_element_type=jnp.float32)
        out[...] = jnp.maximum(total + tower_bias[...], 0.0).astype(jnp.bfloat16)

    def sent(ref, which):
        remote(ref, ref, which, bias_recv.at[0], partner, m).wait_send()

    def all_sent():
        total = others * (groups - 1) + 2
        sent(weights.at[:, pl.ds(0, total * piece), :], 0)
        sent(weights.at[:, pl.ds(0, total * piece), :], 1)
        sent(tower_all.at[pl.ds(0, 5 * depth), :], 2)

        @pl.when(c == 1)
        def _():
            sent(tower_all.at[pl.ds(0, 4 * depth), :], 2)

        sent(outbox.at[pl.ds(0, groups - 1)], 3)
        sent(pooled.at[pl.ds(0, 2)], 4)

        @pl.when(inner)
        def _():
            sent(weights.at[:, pl.ds(0, 2 * piece), :], 0)
            sent(weights.at[:, pl.ds(0, 2 * piece), :], 1)
            sent(pooled.at[pl.ds(0, 2)], 4)

        sent(biases.at[pl.ds(0, others)], 5)

    calls = {
        "P": pool_out,
        "A": pool_away,
        "L": lend,
        "C": corner,
        "F": pass_on,
        "G": share_across,
        "H": share_beside,
        "X": narrow,
    }
    on_units = {"S": spread, "T": pass_and_spread, "R": relay}
    words = {
        "flip": flip,
        "widen": widen,
        "WP": tower_pair,
        "WR": tower_relay,
        "WC": tower_corner,
        "E": ready_all,
        "Y": lift_first,
        "Z": lift_last,
        "end": finish,
    }
    def follow(plan):
        for word in plan:
            if word in words:
                do(words[word])
            elif word[0] in on_units:
                do(on_units[word[0]], *units[int(word[1:])])
            else:
                do(calls[word[0]], *map(int, word[1:]))

    do(first_sends)
    follow(FIRST)

    @pl.when(inner)
    def _():
        follow(INNER)

    @pl.when(jnp.logical_not(inner))
    def _():
        follow(OUTER)

    follow(LAST)
    do(all_sent)


def fused_body(
    feature_ids,
    tables,
    table_of_feature,
    cross_down,
    cross_up,
    cross_bias,
    tower_weight,
    tower_bias,
):
    groups = lax.axis_size("dp")
    members = lax.axis_size("mp")
    _, batch_size, hot_count = feature_ids.shape
    rows = batch_size // (groups * members)
    _, vocab, embed = tables.shape
    layers, block, rank = cross_down.shape
    depth, units = tower_weight.shape
    width = block * members
    pieces = 2 * layers
    dma = pltpu.SemaphoreType.DMA
    anywhere = pl.BlockSpec(memory_space=pl.ANY)
    vmem = pl.BlockSpec(memory_space=pltpu.VMEM)
    return pl.pallas_call(
        functools.partial(kernel, groups, members),
        out_shape=pltpu.VMEM((rows * members, units), jnp.bfloat16),
        in_specs=[anywhere] * 8,
        out_specs=vmem,
        scratch_shapes=[
            pltpu.SMEM((hot_count * batch_size,), jnp.int32),
            pltpu.SMEM(table_of_feature.shape, jnp.int32),
            pltpu.VMEM((vocab, embed), jnp.bfloat16),
            pltpu.VMEM((vocab, embed), jnp.float32),
            pltpu.VMEM((rows, embed), jnp.float32),
            pltpu.VMEM((groups, rows, embed), jnp.bfloat16),
            pltpu.VMEM((members, groups, rows, embed), jnp.bfloat16),
            pltpu.VMEM((rows * members, width), jnp.bfloat16),
            pltpu.VMEM((rows * members, width), jnp.bfloat16),
            pltpu.VMEM((layers, width, rank), jnp.bfloat16),
            pltpu.VMEM((layers, block, rank), jnp.bfloat16),
            pltpu.VMEM((layers, members, rank, block), jnp.bfloat16),
            pltpu.VMEM((members, layers, block), jnp.float32),
            pltpu.VMEM((width, units), jnp.bfloat16),
            pltpu.VMEM((1, units), jnp.float32),
            dma((8,)),
            dma((6,)),
            dma((pieces, members - 1)),
            dma((pieces, members - 1)),
            dma((pieces,)),
            dma((pieces,)),
            dma((4,)),
            dma((2,)),
            dma((members, 2)),
            dma((1,)),
        ],
        compiler_params=pltpu.CompilerParams(
            collective_id=0, has_side_effects=True, vmem_limit_bytes=VMEM_BYTES
        ),
    )(
        feature_ids[0].reshape(-1, LANES, hot_count).transpose(0, 2, 1).reshape(-1),
        table_of_feature,
        tables,
        cross_down,
        cross_up,
        cross_bias,
        tower_weight,
        tower_bias.reshape(1, -1),
    )


def body(
    feature_ids,
    tables,
    table_of_feature,
    cross_down,
    cross_up,
    cross_bias,
    tower_weight,
    tower_bias,
):
    groups = lax.axis_size("dp")
    members = lax.axis_size("mp")
    held = 2 * members * (cross_down.size + cross_up.size) + 2 * groups * tower_weight.size
    placed = groups == 2 * CHIPS and members == PLANES
    even = feature_ids.shape[1] % LANES == 0
    fits = held <= KERNEL_BYTES and placed and even and tables.shape[0] == 1
    chosen = fused_body if fits else plain_body
    return chosen(
        feature_ids,
        tables,
        table_of_feature,
        cross_down,
        cross_up,
        cross_bias,
        tower_weight,
        tower_bias,
    )


def solution(mesh):
    return jax.shard_map(
        body,
        mesh=mesh,
        in_specs=(
            P("dp", None, None),
            P("dp", None, None),
            P(),
            P(None, "mp", None),
            P(None, "mp", None),
            P(None, "mp"),
            P("dp", "mp"),
            P("mp"),
        ),
        out_specs=P("dp", "mp"),
        check_vma=False,
    )
```

```python
import functools

import jax
import jax.numpy as jnp
from jax import lax
from jax.experimental import pallas as pl
from jax.experimental.pallas import tpu as pltpu
from jax.sharding import PartitionSpec as P


def plain_body(
    feature_ids,
    tables,
    table_of_feature,
    cross_down,
    cross_up,
    cross_bias,
    tower_weight,
    tower_bias,
):
    groups = lax.axis_size("dp")
    members = lax.axis_size("mp")
    member = lax.axis_index("mp")
    table_count, batch_size, hot_count = feature_ids.shape
    row_count = batch_size // (groups * members)
    shaped = feature_ids[0].reshape(groups, members, row_count, hot_count)
    own_ids = lax.dynamic_index_in_dim(shaped, member, 1, keepdims=False).reshape(
        groups * row_count, hot_count
    )
    summed = jnp.zeros((groups * row_count, tables.shape[2]), jnp.float32)
    for hot_index in range(hot_count):
        summed = summed + jnp.take(tables[0], own_ids[:, hot_index], axis=0).astype(jnp.float32)
    columns = [summed.astype(jnp.bfloat16)]
    pooled = jnp.stack(columns, axis=1)
    regrouped = lax.all_to_all(pooled, "dp", split_axis=0, concat_axis=1, tiled=True)
    ordered = jnp.take(regrouped, table_of_feature, axis=1)
    by_width = lax.all_to_all(ordered, "mp", split_axis=1, concat_axis=0, tiled=True)
    group_rows = by_width.shape[0]
    embedded = by_width.reshape(group_rows, -1)
    embedded_wide = embedded.astype(jnp.float32)
    crossed = embedded
    layer_total = cross_down.shape[0]
    for layer_index in range(layer_total):
        partial_value = jnp.dot(
            crossed, cross_down[layer_index], preferred_element_type=jnp.float32
        )
        projected = lax.psum(partial_value.astype(jnp.bfloat16), "mp")
        lifted = lax.dot_general(
            projected,
            cross_up[layer_index],
            (((1,), (1,)), ((), ())),
            preferred_element_type=jnp.float32,
        )
        crossed = (
            embedded_wide * (lifted + cross_bias[layer_index]) + crossed.astype(jnp.float32)
        ).astype(jnp.bfloat16)
    full_rows = lax.all_gather(crossed, "mp", axis=1, tiled=True)
    pre_act = jnp.dot(
        full_rows,
        lax.all_gather(tower_weight, "dp", axis=0, tiled=True),
        preferred_element_type=jnp.float32,
    )
    return jax.nn.relu(pre_act + tower_bias).astype(jnp.bfloat16)


MESH = pl.DeviceIdType.MESH
KERNEL_BYTES = 24 * 1024 * 1024
VMEM_BYTES = (64 * 1024 - 352) * 1024
CHIPS = 4
PLANES = 4
LANES = 128
STEPS = (1, 3, 2)
FIRST = (
    "flip", "widen", "P6", "L1", "L2", "L3", "P7", "A6", "P4", "A7", "P5", "A4", "P2", "A5",
)
INNER = (
    "P3", "A2", "P1", "A3", "T1", "T2", "P0", "A1", "S0", "T4", "T5", "S3", "G1", "T7", "T8",
    "G0", "S6", "T10", "T11", "S9", "H1", "H0", "R0", "R1", "R2", "R3", "F11", "R4", "R5",
    "F10", "F01", "R6", "R7", "R8", "R9", "F00", "R10", "R11", "WR", "C0", "C1",
)
OUTER = (
    "P3", "A2", "S0", "P1", "A3", "S3", "P0", "A1", "S6", "S9", "G1", "H1", "G0", "H0", "S1",
    "S2", "R0", "S4", "S5", "R3", "S7", "S8", "R6", "S10", "S11", "R9", "R1", "R2", "R4", "R5",
    "R7", "R8", "R10", "R11", "WR", "C0", "C1",
)
LAST = (
    "C2", "C3", "E", "X0", "Y", "WC", "X1", "Z", "near", "end",
)


def kernel(
    groups,
    members,
    ids_hbm,
    order_hbm,
    table,
    down,
    up,
    bias,
    tower,
    tower_bias_hbm,
    out,
    ids,
    order,
    table_half,
    table_wide,
    sums,
    outbox,
    pooled,
    embedded,
    crossed,
    weights,
    up_raw,
    lifts,
    biases,
    tower_all,
    tower_bias,
    local_sem,
    send_sem,
    z_recv,
    plane_recv,
    diag_recv,
    pair_recv,
    tower_recv,
    pool_recv,
    share_recv,
    bias_recv,
):
    d = lax.axis_index("dp")
    m = lax.axis_index("mp")
    q = lax.div(d, 2)
    c = lax.rem(d, 2)
    partner = q * 2 + 1 - c
    chip_x = q + 1 - 2 * lax.rem(q, 2)
    chip_y = lax.rem(q + 2, CHIPS)
    chip_z = lax.rem(chip_x + 2, CHIPS)
    chips = (chip_x, chip_y, chip_z)
    layers, block, rank = down.shape
    rows, embed = sums.shape
    hots = ids.shape[0] // (rows * groups * members)
    piece = block // groups
    depth = tower.shape[0]
    pieces = 2 * layers
    others = members - 1

    def wrap(value, size):
        return lax.rem(value + size, size)

    def load(src, dst, index):
        copy = pltpu.make_async_copy(src, dst, local_sem.at[index])
        copy.start()
        return copy

    def remote(src, dst, which, recv_sem, to_d, to_m):
        return pltpu.make_async_remote_copy(
            src_ref=src,
            dst_ref=dst,
            send_sem=send_sem.at[which],
            recv_sem=recv_sem,
            device_id=(to_d, to_m),
            device_id_type=MESH,
        )

    def send(src, dst, which, recv_sem, to_d, to_m):
        remote(src, dst, which, recv_sem, to_d, to_m).start()

    def arrived(ref, recv_sem):
        remote(ref, ref, 0, recv_sem, partner, m).wait_recv()

    half_of = lax.div(m, 2)
    beside = m + 1 - 2 * lax.rem(m, 2)
    across = 2 - half_of
    far_first = 2 * (1 - half_of)
    inner = jnp.logical_or(m == 1, m == 2)
    outermost = 3 * (1 - half_of)

    def came(k):
        return (m, beside, across, outermost)[k]

    def goes(k):
        return wrap(m + k, members)

    thin = rank // groups

    def slot(p, member, device, half=None):
        full = piece if p % 2 == 0 else thin
        length = full if half is None else full // 2
        start = device * full + (0 if half is None else half * length)
        if p % 2 == 0:
            start = member * block + start
            return weights.at[p // 2, pl.ds(pl.multiple_of(start, length), length), :]
        return lifts.at[p // 2, member, pl.ds(pl.multiple_of(start, length), length), :]

    def amount(count):
        return weights.at[0, pl.ds(0, count * piece), :]

    def tower_slot(device, half=None):
        length = depth if half is None else depth // 2
        start = device * depth + (0 if half is None else half * length)
        return tower_all.at[pl.ds(pl.multiple_of(start, length), length), :]

    barrier = pltpu.get_barrier_semaphore()
    for k in range(1, members):
        pl.semaphore_signal(barrier, inc=1, device_id=(d, goes(k)), device_id_type=MESH)
    for i in range(1, groups):
        pl.semaphore_signal(barrier, inc=1, device_id=(wrap(d + i, groups), m), device_id_type=MESH)

    here = pl.ds(pl.multiple_of(m * block, block), block)
    tower_copy = load(tower, tower_slot(d), 0)
    down_copy = load(down, weights.at[:, here, :], 1)
    up_copy = load(up, up_raw, 2)
    table_copy = load(table.at[0], table_half, 3)
    ids_copy = load(ids_hbm, ids, 4)
    bias_copy = load(bias, biases.at[m], 5)
    order_copy = load(order_hbm, order, 6)
    tower_bias_copy = load(tower_bias_hbm, tower_bias, 7)

    place = 3 - lax.rem(m + half_of, 2)

    def lend(p):
        mine = slot(p, m, d)
        send(mine, mine, p % 2, z_recv.at[p, place - 1], d, across)
        send(mine, mine, p % 2, z_recv.at[p, 0], d, beside)

    def spread(p, k):
        mine = slot(p, came(k), d)
        arrived(mine, z_recv.at[p, k - 1])
        send(mine, mine, p % 2, plane_recv.at[p, min(k, 2) - 1], chip_x * 2 + c, m)
        send(mine, mine, p % 2, plane_recv.at[p, min(k, 2) - 1], chip_y * 2 + c, m)
        send(mine, mine, p % 2, pair_recv.at[p], partner, m)

    def pass_and_spread(p, k):
        mine = slot(p, came(k), d)
        arrived(mine, z_recv.at[p, k - 1])
        send(mine, mine, p % 2, z_recv.at[p, k - 1], d, beside)
        send(mine, mine, p % 2, plane_recv.at[p, min(k, 2) - 1], chip_x * 2 + c, m)
        send(mine, mine, p % 2, plane_recv.at[p, min(k, 2) - 1], chip_y * 2 + c, m)
        send(mine, mine, p % 2, pair_recv.at[p], partner, m)

    def relay(p, k):
        if k != 2:
            arrived(amount(2 if k == 1 else 4), plane_recv.at[p, min(k, 2) - 1])
        for j in range(2):
            half = slot(p, came(k), chips[j] * 2 + c, j)
            send(half, half, p % 2, diag_recv.at[p], chips[1 - j] * 2 + c, m)
        for j in range(2):
            whole = slot(p, came(k), chips[j] * 2 + c)
            send(whole, whole, p % 2, pair_recv.at[p], partner, m)

    def corner(p):
        arrived(amount(others), diag_recv.at[p])
        for k in STEPS:
            far = slot(p, came(k), chip_z * 2 + c)
            send(far, far, p % 2, pair_recv.at[p], partner, m)

    def complete(p):
        arrived(amount(CHIPS * others), pair_recv.at[p])

    def tower_spread():
        mine = tower_slot(d)
        send(mine, mine, 2, tower_recv.at[0], chip_x * 2 + c, m)
        send(mine, mine, 2, tower_recv.at[0], chip_y * 2 + c, m)
        send(mine, mine, 2, tower_recv.at[2], partner, m)

    def tower_relay():
        arrived(tower_all.at[pl.ds(0, 2 * depth), :], tower_recv.at[0])
        for j in range(2):
            half = tower_slot(chips[j] * 2 + c, j)
            send(half, half, 2, tower_recv.at[1], chips[1 - j] * 2 + c, m)
        for j in range(2):
            whole = tower_slot(chips[j] * 2 + c)
            send(whole, whole, 2, tower_recv.at[2], partner, m)

    def tower_corner():
        far = tower_slot(chip_z * 2 + c)
        arrived(far, tower_recv.at[1])
        send(far, far, 2, tower_recv.at[3], partner, m)

    step = 16 if rows % 16 == 0 else 8

    def pool(group):
        first = (group * members + m) * rows

        def some(index, carry):
            base = pl.multiple_of(index * step, step)
            lane = first + base
            word = lax.div(lane, LANES) * (LANES * hots) + lax.rem(lane, LANES)
            for r in range(step):
                total = None
                for hot in range(hots):
                    at = ids[word + (hot * LANES + r)]
                    row = table_wide[pl.ds(at, 1), :]
                    total = row if total is None else total + row
                sums[pl.ds(base + r, 1), :] = total
            return carry

        lax.fori_loop(0, rows // step, some, 0)
        return sums[...].astype(jnp.bfloat16)

    def related(j):
        return (q, chip_x, chip_y, chip_z)[j // 2] * 2 + (c if j % 2 == 0 else 1 - c)

    def pool_out(j):
        if j == 0:
            pooled[m, 0] = pool(d)
        else:
            outbox[j] = pool(related(j))

    def pool_away(j):
        send(outbox.at[j], pooled.at[m, j], 3, pool_recv.at[j // CHIPS], related(j), m)

    def part(quarter, half):
        return pooled.at[quarter, pl.ds(half * CHIPS, CHIPS)]

    def share_across(half):
        arrived(outbox.at[pl.ds(0, CHIPS - 1 + half)], pool_recv.at[half])
        mine = part(m, half)
        send(mine, mine, 4, share_recv.at[2 * place - 3 + half], d, across)

    def share_beside(half):
        mine = part(m, half)
        send(mine, mine, 4, share_recv.at[0], d, beside)

    def pass_on(far, half):
        quarter = m + 2 - 4 * half_of if far else 3 - m
        theirs = part(quarter, half)
        arrived(theirs, share_recv.at[(3 if far else 1) + half])
        send(theirs, theirs, 4, share_recv.at[(3 if far else 1) + half], d, beside)

    def shared():
        arrived(pooled.at[beside], share_recv.at[0])

        @pl.when(jnp.logical_not(inner))
        def _():
            for quarter, first in ((across, 1), (outermost, 3)):
                for half in range(2):
                    arrived(part(quarter, half), share_recv.at[first + half])

    def embed_all():
        per_block = block // embed
        order_copy.wait()
        for b in range(members):
            for f in range(per_block):
                at = lax.bitwise_xor(order[b * per_block + f], d)
                for quarter in range(members):
                    embedded[
                        b, quarter * rows : (quarter + 1) * rows, f * embed : (f + 1) * embed
                    ] = pooled[quarter, at]

    def project(layer):
        state = embedded if layer == 0 else crossed
        value = None
        for b in range(members):
            term = jnp.dot(
                state[b],
                weights[layer, b * block : (b + 1) * block, :],
                preferred_element_type=jnp.float32,
            )
            value = term if value is None else value + term
        return value.astype(jnp.bfloat16)

    def lift(layer, projected, b):
        state = embedded if layer == 0 else crossed
        lifted = jnp.dot(projected, lifts[layer, b], preferred_element_type=jnp.float32)
        wide = embedded[b].astype(jnp.float32)
        value = wide * (lifted + biases[b, layer : layer + 1, :]) + state[b].astype(jnp.float32)
        return value.astype(jnp.bfloat16)

    units = [(p, k) for p in range(pieces) for k in STEPS]

    def do(call, *args):
        with jax.named_scope(call.__name__ + "_".join(map(str, args))):
            return call(*args)

    def first_sends():
        tower_copy.wait()
        pl.semaphore_wait(barrier, members - 1 + groups - 1)
        tower_spread()
        down_copy.wait()
        lend(0)
        bias_copy.wait()
        for k in range(1, members):
            send(biases.at[m], biases.at[m], 5, bias_recv.at[0], d, goes(k))

    def flip():
        up_copy.wait()
        for n in range(layers):
            lifts[n, m] = up_raw[n].T

    def widen():
        table_copy.wait()
        table_wide[...] = table_half[...].astype(jnp.float32)
        ids_copy.wait()

    state = {}

    def ready():
        shared()
        embed_all()
        arrived(biases.at[pl.ds(0, others)], bias_recv.at[0])

    def narrow(layer):
        complete(2 * layer)
        state["projected"] = project(layer)

    def lift_first():
        complete(1)
        for b in range(members):
            crossed[b] = lift(0, state["projected"], b)

    def lift_last():
        complete(pieces - 1)
        for b in range(members):
            crossed[b] = lift(layers - 1, state["projected"], b)

    def tower_term(b):
        rows_of = pl.ds(pl.multiple_of(b * block, block), block)
        return jnp.dot(crossed[b], tower_all[rows_of, :], preferred_element_type=jnp.float32)

    def near_terms():
        tower_bias_copy.wait()
        arrived(tower_all.at[pl.ds(0, (CHIPS - 1) * depth), :], tower_recv.at[2])
        state["total"] = tower_term(q) + tower_term(chip_x) + tower_term(chip_y)

    def finish():
        arrived(tower_slot(chip_z * 2 + 1 - c), tower_recv.at[3])
        total = state["total"] + tower_term(chip_z)
        out[...] = jnp.maximum(total + tower_bias[...], 0.0).astype(jnp.bfloat16)

    def sent(ref, which):
        remote(ref, ref, which, bias_recv.at[0], partner, m).wait_send()

    def all_sent():
        total = others * (groups - 1) + 2
        sent(weights.at[:, pl.ds(0, total * piece), :], 0)
        sent(weights.at[:, pl.ds(0, total * piece), :], 1)
        sent(tower_all.at[pl.ds(0, 7 * depth), :], 2)
        sent(outbox.at[pl.ds(0, groups - 1)], 3)
        sent(pooled.at[pl.ds(0, 2)], 4)

        @pl.when(inner)
        def _():
            sent(weights.at[:, pl.ds(0, 2 * piece), :], 0)
            sent(weights.at[:, pl.ds(0, 2 * piece), :], 1)
            sent(pooled.at[pl.ds(0, 2)], 4)

        sent(biases.at[pl.ds(0, others)], 5)

    calls = {
        "P": pool_out,
        "A": pool_away,
        "L": lend,
        "C": corner,
        "F": pass_on,
        "G": share_across,
        "H": share_beside,
        "X": narrow,
    }
    on_units = {"S": spread, "T": pass_and_spread, "R": relay}
    words = {
        "flip": flip,
        "widen": widen,
        "WR": tower_relay,
        "WC": tower_corner,
        "E": ready,
        "Y": lift_first,
        "Z": lift_last,
        "near": near_terms,
        "end": finish,
    }
    def follow(plan):
        for word in plan:
            if word in words:
                do(words[word])
            elif word[0] in on_units:
                do(on_units[word[0]], *units[int(word[1:])])
            else:
                do(calls[word[0]], *map(int, word[1:]))

    do(first_sends)
    follow(FIRST)

    @pl.when(inner)
    def _():
        follow(INNER)

    @pl.when(jnp.logical_not(inner))
    def _():
        follow(OUTER)

    follow(LAST)
    do(all_sent)


def fused_body(
    feature_ids,
    tables,
    table_of_feature,
    cross_down,
    cross_up,
    cross_bias,
    tower_weight,
    tower_bias,
):
    groups = lax.axis_size("dp")
    members = lax.axis_size("mp")
    _, batch_size, hot_count = feature_ids.shape
    rows = batch_size // (groups * members)
    _, vocab, embed = tables.shape
    layers, block, rank = cross_down.shape
    depth, units = tower_weight.shape
    width = block * members
    pieces = 2 * layers
    dma = pltpu.SemaphoreType.DMA
    anywhere = pl.BlockSpec(memory_space=pl.ANY)
    vmem = pl.BlockSpec(memory_space=pltpu.VMEM)
    return pl.pallas_call(
        functools.partial(kernel, groups, members),
        out_shape=pltpu.VMEM((rows * members, units), jnp.bfloat16),
        in_specs=[anywhere] * 8,
        out_specs=vmem,
        scratch_shapes=[
            pltpu.SMEM((hot_count * batch_size,), jnp.int32),
            pltpu.SMEM(table_of_feature.shape, jnp.int32),
            pltpu.VMEM((vocab, embed), jnp.bfloat16),
            pltpu.VMEM((vocab, embed), jnp.float32),
            pltpu.VMEM((rows, embed), jnp.float32),
            pltpu.VMEM((groups, rows, embed), jnp.bfloat16),
            pltpu.VMEM((members, groups, rows, embed), jnp.bfloat16),
            pltpu.VMEM((members, rows * members, block), jnp.bfloat16),
            pltpu.VMEM((members, rows * members, block), jnp.bfloat16),
            pltpu.VMEM((layers, width, rank), jnp.bfloat16),
            pltpu.VMEM((layers, block, rank), jnp.bfloat16),
            pltpu.VMEM((layers, members, rank, block), jnp.bfloat16),
            pltpu.VMEM((members, layers, block), jnp.float32),
            pltpu.VMEM((width, units), jnp.bfloat16),
            pltpu.VMEM((1, units), jnp.float32),
            dma((8,)),
            dma((6,)),
            dma((pieces, members - 1)),
            dma((pieces, 2)),
            dma((pieces,)),
            dma((pieces,)),
            dma((4,)),
            dma((2,)),
            dma((5,)),
            dma((1,)),
        ],
        compiler_params=pltpu.CompilerParams(
            collective_id=0, has_side_effects=True, vmem_limit_bytes=VMEM_BYTES
        ),
    )(
        feature_ids[0].reshape(-1, LANES, hot_count).transpose(0, 2, 1).reshape(-1),
        table_of_feature,
        tables,
        cross_down,
        cross_up,
        cross_bias,
        tower_weight,
        tower_bias.reshape(1, -1),
    )


def body(
    feature_ids,
    tables,
    table_of_feature,
    cross_down,
    cross_up,
    cross_bias,
    tower_weight,
    tower_bias,
):
    groups = lax.axis_size("dp")
    members = lax.axis_size("mp")
    held = 2 * members * (cross_down.size + cross_up.size) + 2 * groups * tower_weight.size
    placed = groups == 2 * CHIPS and members == PLANES
    even = feature_ids.shape[1] % LANES == 0
    fits = held <= KERNEL_BYTES and placed and even and tables.shape[0] == 1
    chosen = fused_body if fits else plain_body
    return chosen(
        feature_ids,
        tables,
        table_of_feature,
        cross_down,
        cross_up,
        cross_bias,
        tower_weight,
        tower_bias,
    )


def solution(mesh):
    return jax.shard_map(
        body,
        mesh=mesh,
        in_specs=(
            P("dp", None, None),
            P("dp", None, None),
            P(),
            P(None, "mp", None),
            P(None, "mp", None),
            P(None, "mp"),
            P("dp", "mp"),
            P("mp"),
        ),
        out_specs=P("dp", "mp"),
        check_vma=False,
    )
```
